128 devices in a mesh: gx: 8 (over x_lo, y), gy: 4 (over z), gz: 4 (over x_hi, core).
Axes of the slice: x: 4 (x_hi: 2, x_lo: 2; x = x_hi * 2 + x_lo), y: 4, z: 4, core: 2. Of those that a mesh axis runs over, the one named last changes fastest.
Arguments:
- gas_temp: float32 [128, 512, 1024], P('gz', 'gx', 'gy'), may hold values from 1 to 8
- fuel_frac: float32 [128, 512, 1024], P('gz', 'gx', 'gy'), may hold values from 0 to 1
- velocity: float32 [3, 128, 512, 1024], P(None, 'gz', 'gx', 'gy'), may hold values from -3 to 3
- wall_flags: int32 [512, 1024], P('gx', 'gy'), may hold values 0 or 1
- solid_temp: float32 [64, 1024, 2048], P(None, ('gx', 'gy'), 'gz'), may hold values from 1 to 3
- diffusivity: float32 [64, 1024, 2048], P(None, ('gx', 'gy'), 'gz'), may hold values from 0.03 to 0.15
- gas_owner: int32 [1024, 2048], P(('gx', 'gy'), 'gz'), may hold values from 0 to 524287, as said below
Outputs:
- gas_temp_new: float32 [128, 512, 1024], P('gz', 'gx', 'gy')
- fuel_frac_new: float32 [128, 512, 1024], P('gz', 'gx', 'gy')
- solid_temp_new: float32 [64, 1024, 2048], P(None, ('gx', 'gy'), 'gz')
The draws below stay inside these ranges and needn't reach their ends.
Inputs may be any that keep to these rules, and one draw needn't show every extreme that they name: gas_owner[p, q] = a * 1024 + b where a differs from p // 2 by at most 4 modulo 512 and b differs from q // 2 by at most 4 modulo 1024; both offsets reach 4 in both directions.
All inputs are finite; a program needn't handle non-finite values. No bound on the sum of `wall_flags` on one device may be relied on, other than what follows from the above.
Results may differ from the reference program's by a relative error of at most 0.00002.
Values sent between devices are 32-bit elements; how exact they have to be, the bound alone decides.
A program may use at most 128 MiB of HBM per device.

```python
import math
import jax
import jax.numpy as jnp

SZ = 64
SUBSTEPS = 4
DISP = 4
NX = 512
NY = 1024
NZ = 128
SX = 1024
SY = 2048


def draw_gas_owner(key, part):
    key_rows = jax.random.fold_in(key, 11)
    key_cols = jax.random.fold_in(key, 23)
    shift_rows = jax.random.randint(key_rows, (SX, SY), -DISP, DISP + 1)
    shift_cols = jax.random.randint(key_cols, (SX, SY), -DISP, DISP + 1)
    base_rows = jnp.arange(SX, dtype=jnp.int32)[:, None] // 2
    base_cols = jnp.arange(SY, dtype=jnp.int32)[None, :] // 2
    gas_row = (base_rows + shift_rows) % NX
    gas_col = (base_cols + shift_cols) % NY
    return (gas_row * NY + gas_col).astype(jnp.int32)


def touch_ends(entries, own_key, least, high):
    extent = entries.shape
    spot = [jax.random.randint(jax.random.fold_in(own_key, axis), (), 0, extent[axis]) for axis in range(len(extent))]
    entries = entries.at[tuple(spot)].set(least)
    longest = extent.index(max(extent))
    spot[longest] = (spot[longest] + 1) % extent[longest]
    return entries.at[tuple(spot)].set(high)


def shard_levels(key, extent, pieces, low, largest):
    def one(dim, parts):
        draws = jax.random.uniform(jax.random.fold_in(jax.random.fold_in(key, 6), dim), (parts,), jnp.float32, low / len(pieces), largest / len(pieces))
        return jnp.repeat(jnp.exp(draws), extent[dim] // parts).reshape((-1,) + (1,) * (len(extent) - dim - 1))

    factor_of = one(*pieces[0])
    for cut in pieces[1:]:
        factor_of = factor_of * one(*cut)
    return factor_of


def centred(own_key, shape, spread, bound, split=(), kind=jnp.bfloat16):
    array = jax.random.normal(own_key, shape, jnp.float32) * spread
    if len(split) > 0:
        array = shard_levels(own_key, shape, split, -0.22, 0.18) * array
    return jnp.clip(array, min=-bound, max=bound).astype(kind)


def setup_inputs(seed: int = 0) -> dict:
    keys = jax.random.split(jax.random.key(seed), 8)
    return {
        "gas_temp": jnp.clip(1.0 + 7.0 * jax.random.uniform(keys[0], (NZ, NX, NY), jnp.float32) ** shard_levels(keys[0], (NZ, NX, NY), ((0, 4), (1, 8), (2, 4)), -0.2, 0.2), 1.0, 8.0),
        "fuel_frac": jnp.clip(1.0 * jax.random.uniform(keys[1], (NZ, NX, NY), jnp.float32) ** shard_levels(keys[1], (NZ, NX, NY), ((0, 4), (1, 8), (2, 4)), -0.2, 0.2), 0.0, 1.0),
        "velocity": centred(keys[2], (3, NZ, NX, NY), 0.5, 3.0, ((1, 4), (2, 8), (3, 4)), jnp.float32),
        "wall_flags": touch_ends((jax.random.randint(keys[3], (NX, NY), 0, 4) < 3).astype(jnp.int32), jax.random.fold_in(keys[3], 1), 0, 1),
        "solid_temp": jnp.clip(1.0 + 2.0 * jax.random.uniform(keys[4], (SZ, SX, SY), jnp.float32) ** shard_levels(keys[4], (SZ, SX, SY), ((1, 32), (2, 4)), -0.2, 0.2), 1.0, 3.0),
        "diffusivity": jnp.clip(jnp.exp(math.log(0.15) - 1.609438 * jax.random.uniform(keys[5], (SZ, SX, SY), jnp.float32) ** shard_levels(keys[5], (SZ, SX, SY), ((1, 32), (2, 4)), -0.2, 0.2)), 0.03, 0.15),
        "gas_owner": draw_gas_owner(jax.random.fold_in(keys[7], 71), 0),
    }


FILM_COEF = 0.15
SOURCE_GAIN = 0.25
COOLANT = 1.0
DIFFUSE_TEMP = 0.2
DIFFUSE_FUEL = 0.15
TIME_STEP = 0.2
RATE_CONST = 1.0
ACTIVATION = 4.0
HEAT_RELEASE = 3.0


def gas_update(fields, z_below, z_above, x_below, x_above, y_below, y_above, velocity):
    advect = 0.5 * (velocity[0] * (z_above - z_below) + velocity[1] * (x_above - x_below) + velocity[2] * (y_above - y_below))
    nearby = z_below + z_above + x_below + x_above + y_below + y_above
    reaction = RATE_CONST * fields[1] * jnp.exp(-ACTIVATION / fields[0])
    temp_new = fields[0] + TIME_STEP * (-advect[0] + DIFFUSE_TEMP * (nearby[0] - 6.0 * fields[0]) + HEAT_RELEASE * reaction)
    fuel_new = fields[1] + TIME_STEP * (-advect[1] + DIFFUSE_FUEL * (nearby[1] - 6.0 * fields[1]) - reaction)
    return temp_new, fuel_new


def solid_step(solid_now, diffusivity, wall_flux):
    bottom_ghost = jnp.full_like(solid_now[:1], COOLANT)
    z_below = jnp.concatenate([solid_now[:1], solid_now[:-1]], 0)
    z_above = jnp.concatenate([solid_now[1:], bottom_ghost], 0)
    nearby = z_below + z_above + jnp.roll(solid_now, 1, 1) + jnp.roll(solid_now, -1, 1)
    nearby = nearby + jnp.roll(solid_now, 1, 2) + jnp.roll(solid_now, -1, 2)
    solid_next = solid_now + diffusivity * (nearby - 6.0 * solid_now)
    return solid_next.at[0].add(SOURCE_GAIN * wall_flux)


def reference(gas_temp, fuel_frac, velocity, wall_flags, solid_temp, diffusivity, gas_owner):
    gas_face = gas_temp[0]
    film = FILM_COEF * wall_flags.astype(jnp.float32) * gas_face ** 0.7
    gas_at = gas_face.reshape(-1)[gas_owner]
    film_at = film.reshape(-1)[gas_owner]
    wall_flux = film_at * (gas_at - solid_temp[0])
    solid_now = solid_temp
    for substep in range(SUBSTEPS):
        solid_now = solid_step(solid_now, diffusivity, wall_flux)
    surface = solid_now[0]
    wall_temp = 0.25 * surface.reshape(NX, 2, NY, 2).sum(axis=(1, 3))
    fields = jnp.stack([gas_temp, fuel_frac])
    low_temp = jnp.where(wall_flags == 1, 2.0 * wall_temp - gas_temp[0], gas_temp[0])
    low_layer = jnp.stack([low_temp, fuel_frac[0]])
    z_below = jnp.concatenate([low_layer[:, None], fields[:, :-1]], 1)
    z_above = jnp.concatenate([fields[:, 1:], fields[:, -1:]], 1)
    temp_new, fuel_new = gas_update(fields, z_below, z_above,
                                    jnp.roll(fields, 1, 2), jnp.roll(fields, -1, 2),
                                    jnp.roll(fields, 1, 3), jnp.roll(fields, -1, 3), velocity)
    return temp_new, fuel_new, solid_now
```

```python
import functools

import jax
import jax.numpy as jnp
from jax import lax
from jax.experimental import pallas as pl
from jax.experimental.pallas import tpu as pltpu
from jax.sharding import PartitionSpec as P

MESH = pl.DeviceIdType.MESH
F32 = jnp.float32
I32 = jnp.int32

STEPS = 4
CHUNKS = 4
CL = 16
NL = 64
GL = 32
DISP = 4

PIECES = ((0, 0), (1, 1), (2, -1))
PARTS = (0, 1, 2)


def lane_iota(rows):
    return lax.broadcasted_iota(I32, (rows, 128), 1)


def local(src, dst, sem):
    copy = pltpu.make_async_copy(src, dst, sem)
    copy.start()
    return copy


def kernel(
    gas_ref, fuel_ref, vel_ref, flags_ref, solid_ref, diff_ref, owner_ref,
    gas_out, fuel_out, solid_out,
    G, V, S, D, FL, OW, FS, FB, U, FX,
    WRs, WRr, WCs, WCr, GRs, GRr, GCs, GCr, T0, WTs, WTr,
    lsem, w_send, w_recv, g_send, g_recv, f_send, f_recv, t_send, t_recv,
):
    gx, gy, gz = lax.axis_index("gx"), lax.axis_index("gy"), lax.axis_index("gz")
    row = gx * 4 + gy

    def row_device(r):
        r = lax.rem(r + 32, 32)
        return (lax.div(r, 4), lax.rem(r, 4), gz)

    up_dev = row_device(row - 1)
    down_dev = row_device(row + 1)
    left_dev = (gx, gy, lax.rem(gz + 3, 4))
    right_dev = (gx, gy, lax.rem(gz + 1, 4))
    xm = lax.rem(gx + 7, 8)
    xp = lax.rem(gx + 1, 8)
    gxm_dev = (xm, gy, gz)
    gxp_dev = (xp, gy, gz)
    gym_dev = (gx, lax.rem(gy + 3, 4), gz)
    gyp_dev = (gx, lax.rem(gy + 1, 4), gz)

    loads = {}
    n = 0
    for j in range(2):
        loads["g0", j] = local(
            gas_ref.at[:, :, pl.ds(128 * j, 128)], G.at[0, pl.ds(1, GL), j, pl.ds(8, 64), :], lsem.at[n]
        )
        n += 1
    loads["fl"] = local(flags_ref, FL, lsem.at[n])
    n += 1
    for j in range(4):
        loads["s", j] = local(
            solid_ref.at[:, :, pl.ds(128 * j, 128)], S.at[0, pl.ds(0, NL), j, pl.ds(8, 32), :], lsem.at[n]
        )
        n += 1
    for j in range(2):
        loads["g1", j] = local(
            fuel_ref.at[:, :, pl.ds(128 * j, 128)], G.at[1, pl.ds(1, GL), j, pl.ds(8, 64), :], lsem.at[n]
        )
        n += 1
    loads["ow"] = local(owner_ref, OW, lsem.at[n])
    n += 1
    loads["v"] = local(vel_ref, V, lsem.at[n])
    n += 1
    loads["d"] = local(diff_ref, D, lsem.at[n])

    barrier = pltpu.get_barrier_semaphore()

    def greet(dev):
        pl.semaphore_signal(barrier, inc=1, device_id=dev, device_id_type=MESH)

    for dev in (up_dev, down_dev, left_dev, right_dev, gxm_dev, gxp_dev, gym_dev, gyp_dev):
        greet(dev)
    at_wall = gz == 0
    at_top = gz == 3

    def is_me(a, b, c):
        return (a == gx) & (b == gy) & (c == gz)

    def face_targets():
        out = []
        for piece, shift in PIECES:
            tz = lax.rem(gy + shift + 4, 4)
            for t in range(4):
                self_ = (t == gy) & (tz == 0)
                out.append(((gx, t, tz), piece, 1, 16 * t, self_))
                if t > 0:
                    out.append(((gx, t, tz), piece, 0, 16 * t - 8, self_))
                if t < 3:
                    out.append(((gx, t, tz), piece, 2, 16 * t + 16, self_))
            out.append(((xp, 0, tz), piece, 0, 56, None))
            out.append(((xm, 3, tz), piece, 2, 0, None))
        return out

    def face_devices():
        out = []
        for piece, shift in PIECES:
            tz = lax.rem(gy + shift + 4, 4)
            for t in range(4):
                out.append(((gx, t, tz), (t == gy) & (tz == 0)))
            out.append(((xp, 0, tz), None))
            out.append(((xm, 3, tz), None))
        return out

    count = I32(8)

    @pl.when(at_wall)
    def _():
        for dev, self_ in face_devices():
            if self_ is None:
                greet(dev)
            else:
                pl.when(jnp.logical_not(self_))(functools.partial(greet, dev))

    sources = []
    for piece, shift in PIECES:
        sy = lax.rem(gz - shift + 4, 4)
        self_ = (gz == 0) & (sy == gy)
        sources.append(((gx, sy, 0), self_))
        pl.when(jnp.logical_not(self_))(functools.partial(greet, (gx, sy, 0)))
        pl.when(gy == 0)(functools.partial(greet, (xm, sy, 0)))
        pl.when(gy == 3)(functools.partial(greet, (xp, sy, 0)))
        other = jnp.where(self_, 0, 1) + jnp.where((gy == 0) | (gy == 3), 1, 0)
        count = count + other
    self_sends = I32(0)
    for _, self_ in face_devices():
        if self_ is not None:
            self_sends = self_sends + jnp.where(self_, 1, 0)
    count = count + jnp.where(at_wall, 18 - self_sends, 0)

    S[0, NL] = jnp.ones((4, 48, 128), F32)
    S[1, NL] = jnp.ones((4, 48, 128), F32)

    def send(src, dst, ssem, rsem, dev):
        return pltpu.make_async_remote_copy(
            src_ref=src, dst_ref=dst, send_sem=ssem, recv_sem=rsem, device_id=dev, device_id_type=MESH
        )

    def wall_copies(s, c):
        rows = pl.ds(CL * c, CL)
        return (
            send(WRs.at[s, 0, :, rows, :], WRr.at[s, 1, :, rows, :], w_send.at[s, c, 0], w_recv.at[s, c, 1], up_dev),
            send(WRs.at[s, 1, :, rows, :], WRr.at[s, 0, :, rows, :], w_send.at[s, c, 1], w_recv.at[s, c, 0], down_dev),
            send(WCs.at[s, 0, c], WCr.at[s, 1, c], w_send.at[s, c, 2], w_recv.at[s, c, 3], left_dev),
            send(WCs.at[s, 1, c], WCr.at[s, 0, c], w_send.at[s, c, 3], w_recv.at[s, c, 2], right_dev),
        )

    lane32 = lane_iota(32)
    lane64 = lane_iota(64)

    for j in range(4):
        loads["s", j].wait()

    for c in range(CHUNKS):
        def pack(i, carry, c=c):
            cl, cr = carry
            l = CL * c + i
            for j in range(4):
                WRs[0, 0, j, pl.ds(l, 1), :] = S[0, l, j, 8:9, :]
                WRs[0, 1, j, pl.ds(l, 1), :] = S[0, l, j, 39:40, :]
            cl = jnp.where(lane32 == i, pltpu.roll(S[0, l, 0, 8:40, :], i, 1), cl)
            cr = jnp.where(lane32 == i, pltpu.roll(S[0, l, 3, 8:40, :], i + 1, 1), cr)
            return cl, cr

        zero = jnp.zeros((32, 128), F32)
        cl, cr = lax.fori_loop(0, CL, pack, (zero, zero))
        WCs[0, 0, c] = cl
        WCs[0, 1, c] = cr

    for key in (("g0", 0), ("g0", 1), "fl", ("g1", 0), ("g1", 1)):
        loads[key].wait()
    for j in range(2):
        FS[0, j] = G[0, 1, j, 8:72, :]
        FS[1, j] = FL[:, 128 * j : 128 * j + 128].astype(F32)

    def gpack(l, carry):
        cl, cr = carry
        for f in range(2):
            for j in range(2):
                GRs[0, f, j, pl.ds(l, 1), :] = G[f, l + 1, j, 8:9, :]
                GRs[1, f, j, pl.ds(l, 1), :] = G[f, l + 1, j, 71:72, :]
            i = f * GL + l
            cl = jnp.where(lane64 == i, pltpu.roll(G[f, l + 1, 0, 8:72, :], i, 1), cl)
            cr = jnp.where(lane64 == i, pltpu.roll(G[f, l + 1, 1, 8:72, :], i + 1, 1), cr)
        return cl, cr

    zero = jnp.zeros((64, 128), F32)
    cl, cr = lax.fori_loop(0, GL, gpack, (zero, zero))
    GCs[0] = cl
    GCs[1] = cr

    pl.semaphore_wait(barrier, count)

    for c in reversed(range(CHUNKS)):
        for copy in wall_copies(0, c):
            copy.start()

    def face_ref(buf, piece):
        return buf.at[:, pl.ds(1, 2)] if piece == 0 else buf.at[:, pl.ds(0 if piece == 1 else 3, 1)]

    def face_source(piece):
        return FS if piece == 0 else FS.at[:, pl.ds(1 if piece == 1 else 0, 1)]

    PART = ((0, 8), (8, 16), (24, 8))

    def face_copy(n, dev, piece, part, r):
        start, size = PART[part]
        return send(
            face_source(piece).at[:, :, pl.ds(r, size), :],
            face_ref(FB, piece).at[:, :, pl.ds(start, size), :],
            f_send.at[n],
            f_recv.at[piece, part],
            dev,
        )

    def face_here(piece, part, r):
        start, size = PART[part]
        if piece == 0:
            FB[:, 1:3, start : start + size, :] = FS[:, :, r : r + size, :]
        elif piece == 1:
            FB[:, 0, start : start + size, :] = FS[:, 1, r : r + size, :]
        else:
            FB[:, 3, start : start + size, :] = FS[:, 0, r : r + size, :]

    @pl.when(at_wall)
    def _():
        for n, (dev, piece, part, r, self_) in enumerate(face_targets()):
            copy = face_copy(n, dev, piece, part, r)
            if self_ is None:
                copy.start()
            else:
                pl.when(jnp.logical_not(self_))(copy.start)
                pl.when(self_)(functools.partial(face_here, piece, part, r))

    g_copies = (
        send(GRs.at[0], GRr.at[1], g_send.at[0], g_recv.at[1], gxm_dev),
        send(GRs.at[1], GRr.at[0], g_send.at[1], g_recv.at[0], gxp_dev),
        send(GCs.at[0], GCr.at[1], g_send.at[2], g_recv.at[3], gym_dev),
        send(GCs.at[1], GCr.at[0], g_send.at[3], g_recv.at[2], gyp_dev),
    )
    for copy in g_copies:
        copy.start()
    z_down = send(
        G.at[:, 1, :, pl.ds(8, 64), :], G.at[:, GL + 1, :, pl.ds(8, 64), :], g_send.at[4], g_recv.at[5], left_dev
    )
    z_up = send(
        G.at[:, GL, :, pl.ds(8, 64), :], G.at[:, 0, :, pl.ds(8, 64), :], g_send.at[5], g_recv.at[4], right_dev
    )
    pl.when(jnp.logical_not(at_wall))(z_down.start)
    pl.when(jnp.logical_not(at_top))(z_up.start)

    def gas_layer(l):
        g = l + 1
        for f in range(2):
            for j in range(2):
                G[f, g, j, 7:8, :] = GRr[0, f, j, pl.ds(l, 1), :]
                G[f, g, j, 72:73, :] = GRr[1, f, j, pl.ds(l, 1), :]
        RB = 16
        lane = lane_iota(RB)
        for b in range(64 // RB):
            r0 = 8 + RB * b
            rows = slice(r0, r0 + RB)
            out = slice(RB * b, RB * b + RB)
            sums, advs, mids = {}, {}, {}
            vels = [[V[d, l, out, 128 * j : 128 * j + 128] for j in range(2)] for d in range(3)]
            for f in range(2):
                i = f * GL + l
                mid = [G[f, g, j, rows, :] for j in range(2)]
                lo = [pltpu.roll(GCr[0, out, :], lax.rem(128 - i, 128), 1)] + [pltpu.roll(m, 1, 1) for m in mid]
                hi = [pltpu.roll(m, 127, 1) for m in mid] + [pltpu.roll(GCr[1, out, :], 127 - i, 1)]
                for j in range(2):
                    y_lo = jnp.where(lane == 0, lo[j], lo[j + 1])
                    y_hi = jnp.where(lane == 127, hi[j + 1], hi[j])
                    x_lo = G[f, g, j, r0 - 1 : r0 - 1 + RB, :]
                    x_hi = G[f, g, j, r0 + 1 : r0 + 1 + RB, :]
                    z_lo = G[f, g - 1, j, rows, :]
                    z_hi = G[f, g + 1, j, rows, :]
                    sums[f, j] = ((z_lo + z_hi) + (x_lo + x_hi)) + (y_lo + y_hi)
                    advs[f, j] = 0.5 * (
                        vels[0][j] * (z_hi - z_lo) + vels[1][j] * (x_hi - x_lo) + vels[2][j] * (y_hi - y_lo)
                    )
                    mids[f, j] = mid[j]
            for j in range(2):
                temp, fuel = mids[0, j], mids[1, j]
                reaction = fuel * jnp.exp(-4.0 / temp)
                lanes = slice(128 * j, 128 * j + 128)
                gas_out[l, out, lanes] = temp + 0.2 * (
                    0.2 * (sums[0, j] - 6.0 * temp) - advs[0, j] + 3.0 * reaction
                )
                fuel_out[l, out, lanes] = fuel + 0.2 * (
                    0.15 * (sums[1, j] - 6.0 * fuel) - advs[1, j] - reaction
                )

    def gas_layers(first, last):
        def body(l, carry):
            gas_layer(l)
            return carry

        lax.fori_loop(first, last, body, 0)

    def wall_layer(s, c, i, PL, PR, cl, cr, flux):
        l = CL * c + i
        src, dst = S.at[s % 2], S.at[(s + 1) % 2]
        lm = l - 1 if not flux else l
        for j in range(4):
            src[l, j, 7:8, :] = WRr[s, 0, j, pl.ds(l, 1), :]
            src[l, j, 40:41, :] = WRr[s, 1, j, pl.ds(l, 1), :]
        mid = [src[l, j, 8:40, :] for j in range(4)]
        lo = [pltpu.roll(PL, lax.rem(128 - i, 128), 1)] + [pltpu.roll(m, 1, 1) for m in mid]
        hi = [pltpu.roll(m, 127, 1) for m in mid] + [pltpu.roll(PR, 127 - i, 1)]
        for j in range(4):
            y_lo = jnp.where(lane32 == 0, lo[j], lo[j + 1])
            y_hi = jnp.where(lane32 == 127, hi[j + 1], hi[j])
            near = (src[lm, j, 8:40, :] + src[l + 1, j, 8:40, :]) + (src[l, j, 7:39, :] + src[l, j, 9:41, :])
            near = near + (y_lo + y_hi)
            lanes = slice(128 * j, 128 * j + 128)
            new = mid[j] + D[l, :, lanes] * (near - 6.0 * mid[j])
            if flux:
                new = new + FX[j]
            if s == STEPS - 1:
                solid_out[l, :, lanes] = new
                if flux:
                    T0[j] = new
            else:
                dst[l, j, 8:40, :] = new
                WRs[s + 1, 0, j, pl.ds(l, 1), :] = new[0:1, :]
                WRs[s + 1, 1, j, pl.ds(l, 1), :] = new[31:32, :]
                if j == 0:
                    cl = jnp.where(lane32 == i, pltpu.roll(new, i, 1), cl)
                if j == 3:
                    cr = jnp.where(lane32 == i, pltpu.roll(new, i + 1, 1), cr)
        return cl, cr

    def wall_chunk(s, c):
        for copy in wall_copies(s, c):
            copy.wait_recv()
        PL, PR = WCr[s, 0, c], WCr[s, 1, c]
        cl = cr = jnp.zeros((32, 128), F32)
        first = 0
        if c == 0:
            cl, cr = wall_layer(s, c, I32(0), PL, PR, cl, cr, True)
            first = 1

        def body(i, carry):
            return wall_layer(s, c, i, PL, PR, *carry, False)

        cl, cr = lax.fori_loop(first, CL, body, (cl, cr))
        if s < STEPS - 1:
            WCs[s + 1, 0, c] = cl
            WCs[s + 1, 1, c] = cr
            for copy in wall_copies(s + 1, c):
                copy.start()

    def wall_flux():
        for piece, (dev, self_) in enumerate(sources):
            for part in PARTS:
                copy = face_copy(0, dev, piece, part, 0)
                here = self_
                if part == 0:
                    here = self_ & (gy > 0)
                if part == 2:
                    here = self_ & (gy < 3)
                pl.when(jnp.logical_not(here))(copy.wait_recv)
        tiles = [jnp.where(FB[1, j] > 0.5, FB[0, j], -FB[0, j]) for j in range(4)]
        prow = lax.broadcasted_iota(I32, (32, 128), 0)
        half = row * 16 + lax.shift_right_logical(prow, 1)
        for k in range(4):
            if k % 2 == 0:
                a, b, shift, cut = k // 2, k // 2 + 1, 32, 32
            else:
                a, b, shift, cut = k // 2 + 1, k // 2 + 2, 96, 96
            a, b = ((0, 1), (1, 2), (1, 2), (2, 3))[k]
            window = jnp.where(lane32 < cut, pltpu.roll(tiles[a], shift, 1), pltpu.roll(tiles[b], shift, 1))
            U[pl.ds(0, 32, stride=2), :] = window
            U[pl.ds(1, 32, stride=2), :] = window
            own = OW[:, 128 * k : 128 * k + 128]
            arow = lax.shift_right_logical(own, 10)
            acol = lax.bitwise_and(own, 1023)
            shift_row = lax.bitwise_and(arow - half + DISP, 511)
            col = lax.bitwise_and(acol - (gz * 256 - 128), 1023) - (96 + 64 * k)
            value = jnp.zeros((32, 128), F32)
            for d in range(2 * DISP + 1):
                base = 16 + 2 * (d - DISP)
                picked = jnp.take_along_axis(U[base : base + 32, :], col, axis=1, mode="promise_in_bounds")
                value = jnp.where(shift_row == d, picked, value)
            gas_at = jnp.abs(value)
            film = jnp.where(value > 0.0, 0.15 * jnp.exp(0.7 * jnp.log(gas_at)), 0.0)
            FX[k] = 0.25 * (film * (gas_at - S[0, 0, k, 8:40, :]))

    loads["d"].wait()
    loads["ow"].wait()
    for c in (3, 2, 1):
        wall_chunk(0, c)
    wall_flux()
    wall_chunk(0, 0)
    loads["v"].wait()
    for copy in g_copies:
        copy.wait_recv()
    pl.when(jnp.logical_not(at_top))(z_down.wait_recv)

    @pl.when(at_top)
    def _():
        for f in range(2):
            for j in range(2):
                G[f, GL + 1, j, 8:72, :] = G[f, GL, j, 8:72, :]

    gas_layers(1, 9)
    for c in (3, 2, 1, 0):
        wall_chunk(1, c)
    gas_layers(9, 17)
    for c in (3, 2, 1, 0):
        wall_chunk(2, c)
    gas_layers(17, 25)
    for c in (0, 1, 2, 3):
        wall_chunk(3, c)

    lane16 = lane_iota(16)
    idx = lax.bitwise_and(2 * lane16, 127)
    for k in range(2):
        halves = []
        for j in (2 * k, 2 * k + 1):
            y = T0[j, pl.ds(0, 16, stride=2), :] + T0[j, pl.ds(1, 16, stride=2), :]
            y = 0.25 * (y + pltpu.roll(y, 127, 1))
            halves.append(jnp.take_along_axis(y, idx, axis=1, mode="promise_in_bounds"))
        WTs[k] = jnp.where(lane16 < 64, halves[0], halves[1])
    wt_self = (gz == 0) & (gy == 0)
    wt_rows = pl.ds(pl.multiple_of(gy * 16, 16), 16)
    wt_copy = send(WTs, WTr.at[:, wt_rows, :], t_send, t_recv.at[gy], (gx, gz, 0))
    pl.when(jnp.logical_not(wt_self))(wt_copy.start)

    @pl.when(wt_self)
    def _():
        WTr[:, 0:16, :] = WTs[...]

    gas_layers(25, GL)

    @pl.when(jnp.logical_not(at_wall))
    def _():
        z_up.wait_recv()

    @pl.when(at_wall)
    def _():
        for t in range(4):
            copy = send(WTs, WTr.at[:, pl.ds(16 * t, 16), :], t_send, t_recv.at[t], (gx, t, gy))
            here = (gy == 0) & (t == 0)
            pl.when(jnp.logical_not(here))(copy.wait_recv)
        for j in range(2):
            temp = G[0, 1, j, 8:72, :]
            G[0, 0, j, 8:72, :] = jnp.where(FS[1, j] > 0.5, 2.0 * WTr[j] - temp, temp)
            G[1, 0, j, 8:72, :] = G[1, 1, j, 8:72, :]

    gas_layers(0, 1)

    for s in range(STEPS):
        for c in range(CHUNKS):
            for copy in wall_copies(s, c):
                copy.wait_send()
    for copy in g_copies:
        copy.wait_send()
    pl.when(jnp.logical_not(at_wall))(z_down.wait_send)
    pl.when(jnp.logical_not(at_top))(z_up.wait_send)
    pl.when(jnp.logical_not(wt_self))(wt_copy.wait_send)

    @pl.when(at_wall)
    def _():
        for n, (dev, piece, part, r, self_) in enumerate(face_targets()):
            copy = face_copy(n, dev, piece, part, r)
            if self_ is None:
                copy.wait_send()
            else:
                pl.when(jnp.logical_not(self_))(copy.wait_send)


def shards(gas_temp, fuel_frac, velocity, wall_flags, solid_temp, diffusivity, gas_owner):
    hbm = pl.BlockSpec(memory_space=pltpu.HBM)
    vmem = pl.BlockSpec(memory_space=pltpu.VMEM)
    gas_shape, solid_shape = gas_temp.shape, solid_temp.shape
    dma = pltpu.SemaphoreType.DMA
    buf = pltpu.VMEM
    results = [gas_shape, gas_shape, solid_shape]
    return pl.pallas_call(
        kernel,
        out_shape=[pltpu.VMEM(s, F32) for s in results],
        in_specs=[hbm] * 7,
        out_specs=[vmem] * 3,
        scratch_shapes=[
            buf((2, GL + 2, 2, 80, 128), F32),
            buf((3, GL, 64, 256), F32),
            buf((2, NL + 1, 4, 48, 128), F32),
            buf((NL, 32, 512), F32),
            buf((64, 256), I32),
            buf((32, 512), I32),
            buf((2, 2, 64, 128), F32),
            buf((2, 4, 32, 128), F32),
            buf((64, 128), F32),
            buf((4, 32, 128), F32),
            buf((STEPS, 2, 4, NL, 128), F32),
            buf((STEPS, 2, 4, NL, 128), F32),
            buf((STEPS, 2, CHUNKS, 32, 128), F32),
            buf((STEPS, 2, CHUNKS, 32, 128), F32),
            buf((2, 2, 2, GL, 128), F32),
            buf((2, 2, 2, GL, 128), F32),
            buf((2, 64, 128), F32),
            buf((2, 64, 128), F32),
            buf((4, 32, 128), F32),
            buf((2, 16, 128), F32),
            buf((2, 64, 128), F32),
            dma((12,)),
            dma((STEPS, CHUNKS, 4)),
            dma((STEPS, CHUNKS, 4)),
            dma((6,)),
            dma((6,)),
            dma((36,)),
            dma((3, 3)),
            dma,
            dma((4,)),
        ],
        compiler_params=pltpu.CompilerParams(
            collective_id=0, has_side_effects=True, vmem_limit_bytes=52 * 1024 * 1024
        ),
        name="section",
    )(gas_temp, fuel_frac, velocity, wall_flags, solid_temp, diffusivity, gas_owner)


def solution(mesh):
    placed = (
        P("gz", "gx", "gy"),
        P("gz", "gx", "gy"),
        P(None, "gz", "gx", "gy"),
        P("gx", "gy"),
        P(None, ("gx", "gy"), "gz"),
        P(None, ("gx", "gy"), "gz"),
        P(("gx", "gy"), "gz"),
    )
    return jax.shard_map(
        shards,
        mesh=mesh,
        in_specs=placed,
        out_specs=(P("gz", "gx", "gy"), P("gz", "gx", "gy"), P(None, ("gx", "gy"), "gz")),
        check_vma=False,
    )
```

```python
import functools

import jax
import jax.numpy as jnp
from jax import lax
from jax.experimental import pallas as pl
from jax.experimental.pallas import tpu as pltpu
from jax.sharding import PartitionSpec as P

MESH = pl.DeviceIdType.MESH
F32 = jnp.float32
I32 = jnp.int32

STEPS = 4
CHUNKS = 4
CL = 16
NL = 64
WU = 4
PU = 4
GAS_1 = 13
GAS_2 = 21
GL = 32
DISP = 4

PIECES = ((0, 0), (1, 1), (2, -1))
PARTS = (0, 1, 2)


def lane_iota(rows):
    return lax.broadcasted_iota(I32, (rows, 128), 1)


def local(src, dst, sem):
    copy = pltpu.make_async_copy(src, dst, sem)
    copy.start()
    return copy


def kernel(
    gas_ref, fuel_ref, vel_ref, flags_ref, solid_ref, diff_ref, owner_ref,
    gas_out, fuel_out, solid_out,
    G, V, S, D, FL, OW, FS, FB, U, FX,
    WRs, WRr, WCs, WCr, WC, GRs, GRr, GCs, GCr, GC, T0, WTs, WTr,
    lsem, w_send, w_recv, g_send, g_recv, f_send, f_recv, t_send, t_recv,
):
    gx, gy, gz = lax.axis_index("gx"), lax.axis_index("gy"), lax.axis_index("gz")
    row = gx * 4 + gy

    def row_device(r):
        r = lax.rem(r + 32, 32)
        return (lax.div(r, 4), lax.rem(r, 4), gz)

    up_dev = row_device(row - 1)
    down_dev = row_device(row + 1)
    left_dev = (gx, gy, lax.rem(gz + 3, 4))
    right_dev = (gx, gy, lax.rem(gz + 1, 4))
    xm = lax.rem(gx + 7, 8)
    xp = lax.rem(gx + 1, 8)
    gxm_dev = (xm, gy, gz)
    gxp_dev = (xp, gy, gz)
    gym_dev = (gx, lax.rem(gy + 3, 4), gz)
    gyp_dev = (gx, lax.rem(gy + 1, 4), gz)

    loads = {}
    n = 0
    for j in range(2):
        loads["g0", j] = local(
            gas_ref.at[:, :, pl.ds(128 * j, 128)], G.at[0, pl.ds(1, GL), j, pl.ds(8, 64), :], lsem.at[n]
        )
        n += 1
    loads["fl"] = local(flags_ref, FL, lsem.at[n])
    n += 1
    for j in range(4):
        loads["s", j] = local(
            solid_ref.at[:, :, pl.ds(128 * j, 128)], S.at[0, pl.ds(0, NL), j, pl.ds(8, 32), :], lsem.at[n]
        )
        n += 1
    for j in range(2):
        loads["g1", j] = local(
            fuel_ref.at[:, :, pl.ds(128 * j, 128)], G.at[1, pl.ds(1, GL), j, pl.ds(8, 64), :], lsem.at[n]
        )
        n += 1
    loads["ow"] = local(owner_ref, OW, lsem.at[n])
    n += 1
    loads["v"] = local(vel_ref, V, lsem.at[n])
    n += 1
    loads["d"] = local(diff_ref, D, lsem.at[n])

    barrier = pltpu.get_barrier_semaphore()

    def greet(dev):
        pl.semaphore_signal(barrier, inc=1, device_id=dev, device_id_type=MESH)

    for dev in (up_dev, down_dev, left_dev, right_dev, gxm_dev, gxp_dev, gym_dev, gyp_dev):
        greet(dev)
    at_wall = gz == 0
    at_top = gz == 3

    def is_me(a, b, c):
        return (a == gx) & (b == gy) & (c == gz)

    def face_targets():
        out = []
        for piece, shift in PIECES:
            tz = lax.rem(gy + shift + 4, 4)
            for t in range(4):
                self_ = (t == gy) & (tz == 0)
                out.append(((gx, t, tz), piece, 1, 16 * t, self_))
                if t > 0:
                    out.append(((gx, t, tz), piece, 0, 16 * t - 8, self_))
                if t < 3:
                    out.append(((gx, t, tz), piece, 2, 16 * t + 16, self_))
            out.append(((xp, 0, tz), piece, 0, 56, None))
            out.append(((xm, 3, tz), piece, 2, 0, None))
        return out

    def face_devices():
        out = []
        for piece, shift in PIECES:
            tz = lax.rem(gy + shift + 4, 4)
            for t in range(4):
                out.append(((gx, t, tz), (t == gy) & (tz == 0)))
            out.append(((xp, 0, tz), None))
            out.append(((xm, 3, tz), None))
        return out

    count = I32(8)

    @pl.when(at_wall)
    def _():
        for dev, self_ in face_devices():
            if self_ is None:
                greet(dev)
            else:
                pl.when(jnp.logical_not(self_))(functools.partial(greet, dev))

    sources = []
    for piece, shift in PIECES:
        sy = lax.rem(gz - shift + 4, 4)
        self_ = (gz == 0) & (sy == gy)
        sources.append(((gx, sy, 0), self_))
        pl.when(jnp.logical_not(self_))(functools.partial(greet, (gx, sy, 0)))
        pl.when(gy == 0)(functools.partial(greet, (xm, sy, 0)))
        pl.when(gy == 3)(functools.partial(greet, (xp, sy, 0)))
        other = jnp.where(self_, 0, 1) + jnp.where((gy == 0) | (gy == 3), 1, 0)
        count = count + other
    self_sends = I32(0)
    for _, self_ in face_devices():
        if self_ is not None:
            self_sends = self_sends + jnp.where(self_, 1, 0)
    count = count + jnp.where(at_wall, 18 - self_sends, 0)

    S[0, NL] = jnp.ones((4, 48, 128), F32)
    S[1, NL] = jnp.ones((4, 48, 128), F32)

    def send(src, dst, ssem, rsem, dev):
        return pltpu.make_async_remote_copy(
            src_ref=src, dst_ref=dst, send_sem=ssem, recv_sem=rsem, device_id=dev, device_id_type=MESH
        )

    def wall_copies(s, c):
        rows = pl.ds(c * CL if isinstance(c, int) else pl.multiple_of(c * CL, CL), CL)
        return (
            send(WRs.at[s, 0, :, rows, :], WRr.at[s, 1, :, rows, :], w_send.at[s, c, 0], w_recv.at[s, c, 1], up_dev),
            send(WRs.at[s, 1, :, rows, :], WRr.at[s, 0, :, rows, :], w_send.at[s, c, 1], w_recv.at[s, c, 0], down_dev),
            send(WCs.at[s, c], WCr.at[s, 1, c], w_send.at[s, c, 2], w_recv.at[s, c, 3], left_dev),
            send(WCs.at[s, c], WCr.at[s, 0, c], w_send.at[s, c, 3], w_recv.at[s, c, 2], right_dev),
        )

    lane32 = lane_iota(32)
    lane64 = lane_iota(64)

    for j in range(4):
        loads["s", j].wait()

    zero32 = jnp.zeros((32, 128), F32)

    def columns(acc, first, last, i, lane):
        both = pltpu.roll(jnp.where(lane < 64, first, last), 2 * i + 1, 1)
        return jnp.where(lax.shift_right_arithmetic(lane, 1) == i, both, acc)

    def pack_chunk(c, carry):
        def pack(n, acc):
            for k in range(PU):
                i = PU * n + k
                l = CL * c + i
                for j in range(4):
                    WRs[0, 0, j, pl.ds(l, 1), :] = S[0, l, j, 8:9, :]
                    WRs[0, 1, j, pl.ds(l, 1), :] = S[0, l, j, 39:40, :]
                acc = columns(acc, S[0, l, 0, 8:40, :], S[0, l, 3, 8:40, :], i, lane32)
            return acc

        WCs[0, c] = lax.fori_loop(0, CL // PU, pack, zero32)
        return carry

    lax.fori_loop(0, CHUNKS, pack_chunk, 0)

    for key in (("g0", 0), ("g0", 1), "fl", ("g1", 0), ("g1", 1)):
        loads[key].wait()
    for j in range(2):
        FS[0, j] = G[0, 1, j, 8:72, :]
        FS[1, j] = FL[:, 128 * j : 128 * j + 128].astype(F32)

    def gpack(n, acc):
        for k in range(2):
            l = 2 * n + k
            for f in range(2):
                for j in range(2):
                    GRs[0, f, j, pl.ds(l, 1), :] = G[f, l + 1, j, 8:9, :]
                    GRs[1, f, j, pl.ds(l, 1), :] = G[f, l + 1, j, 71:72, :]
                acc = columns(acc, G[f, l + 1, 0, 8:72, :], G[f, l + 1, 1, 8:72, :], f * GL + l, lane64)
        return acc

    GCs[...] = lax.fori_loop(0, GL // 2, gpack, jnp.zeros((64, 128), F32))

    pl.semaphore_wait(barrier, count)

    def face_ref(buf, piece):
        return buf.at[:, pl.ds(1, 2)] if piece == 0 else buf.at[:, pl.ds(0 if piece == 1 else 3, 1)]

    def face_source(piece):
        return FS if piece == 0 else FS.at[:, pl.ds(1 if piece == 1 else 0, 1)]

    PART = ((0, 8), (8, 16), (24, 8))

    def face_copy(n, dev, piece, part, r):
        start, size = PART[part]
        return send(
            face_source(piece).at[:, :, pl.ds(r, size), :],
            face_ref(FB, piece).at[:, :, pl.ds(start, size), :],
            f_send.at[n],
            f_recv.at[piece, part],
            dev,
        )

    def face_here(piece, part, r):
        start, size = PART[part]
        if piece == 0:
            FB[:, 1:3, start : start + size, :] = FS[:, :, r : r + size, :]
        elif piece == 1:
            FB[:, 0, start : start + size, :] = FS[:, 1, r : r + size, :]
        else:
            FB[:, 3, start : start + size, :] = FS[:, 0, r : r + size, :]

    g_copies = (
        send(GRs.at[0], GRr.at[1], g_send.at[0], g_recv.at[1], gxm_dev),
        send(GRs.at[1], GRr.at[0], g_send.at[1], g_recv.at[0], gxp_dev),
        send(GCs, GCr.at[1], g_send.at[2], g_recv.at[3], gym_dev),
        send(GCs, GCr.at[0], g_send.at[3], g_recv.at[2], gyp_dev),
    )
    for copy in g_copies:
        copy.start()
    for c in reversed(range(CHUNKS)):
        for copy in wall_copies(0, c):
            copy.start()

    @pl.when(at_wall)
    def _():
        for n, (dev, piece, part, r, self_) in enumerate(face_targets()):
            copy = face_copy(n, dev, piece, part, r)
            if self_ is None:
                copy.start()
            else:
                pl.when(jnp.logical_not(self_))(copy.start)
                pl.when(self_)(functools.partial(face_here, piece, part, r))

    z_down = send(
        G.at[:, 1, :, pl.ds(8, 64), :], G.at[:, GL + 1, :, pl.ds(8, 64), :], g_send.at[4], g_recv.at[5], left_dev
    )
    z_up = send(
        G.at[:, GL, :, pl.ds(8, 64), :], G.at[:, 0, :, pl.ds(8, 64), :], g_send.at[5], g_recv.at[4], right_dev
    )
    pl.when(jnp.logical_not(at_wall))(z_down.start)
    pl.when(jnp.logical_not(at_top))(z_up.start)

    def gas_layer(l):
        g = l + 1
        for f in range(2):
            for j in range(2):
                G[f, g, j, 7:8, :] = GRr[0, f, j, pl.ds(l, 1), :]
                G[f, g, j, 72:73, :] = GRr[1, f, j, pl.ds(l, 1), :]
        RB = 16
        lane = lane_iota(RB)
        for b in range(64 // RB):
            r0 = 8 + RB * b
            rows = slice(r0, r0 + RB)
            out = slice(RB * b, RB * b + RB)
            sums, advs, mids = {}, {}, {}
            vels = [[V[d, l, out, 128 * j : 128 * j + 128] for j in range(2)] for d in range(3)]
            for f in range(2):
                i = f * GL + l
                mid = [G[f, g, j, rows, :] for j in range(2)]
                edge = pltpu.roll(GC[out, :], lax.bitwise_and(128 - 2 * i, 127), 1)
                lo = [edge] + [pltpu.roll(m, 1, 1) for m in mid]
                hi = [pltpu.roll(m, 127, 1) for m in mid] + [edge]
                for j in range(2):
                    y_lo = jnp.where(lane == 0, lo[j], lo[j + 1])
                    y_hi = jnp.where(lane == 127, hi[j + 1], hi[j])
                    x_lo = G[f, g, j, r0 - 1 : r0 - 1 + RB, :]
                    x_hi = G[f, g, j, r0 + 1 : r0 + 1 + RB, :]
                    z_lo = G[f, g - 1, j, rows, :]
                    z_hi = G[f, g + 1, j, rows, :]
                    sums[f, j] = ((z_lo + z_hi) + (x_lo + x_hi)) + (y_lo + y_hi)
                    advs[f, j] = 0.5 * (
                        vels[0][j] * (z_hi - z_lo) + vels[1][j] * (x_hi - x_lo) + vels[2][j] * (y_hi - y_lo)
                    )
                    mids[f, j] = mid[j]
            for j in range(2):
                temp, fuel = mids[0, j], mids[1, j]
                reaction = fuel * jnp.exp(-4.0 / temp)
                lanes = slice(128 * j, 128 * j + 128)
                gas_out[l, out, lanes] = temp + 0.2 * (
                    0.2 * (sums[0, j] - 6.0 * temp) - advs[0, j] + 3.0 * reaction
                )
                fuel_out[l, out, lanes] = fuel + 0.2 * (
                    0.15 * (sums[1, j] - 6.0 * fuel) - advs[1, j] - reaction
                )

    def gas_layers(first, last):
        def body(l, carry):
            gas_layer(l)
            return carry

        lax.fori_loop(first, last, body, 0)

    def wall_pack(s, c, g, acc):
        dst = S.at[(s + 1) % 2]
        for k in range(WU):
            i = WU * g + k
            l = jnp.maximum(CL * c + i, 0)
            acc = columns(acc, dst[l, 0, 8:40, :], dst[l, 3, 8:40, :], i, lane32)
        return acc

    def wall_group(s, c, g, acc):
        src, dst = S.at[s % 2], S.at[(s + 1) % 2]
        if s < STEPS - 1:
            acc = wall_pack(s, c, g - 1, acc)
        for k in range(WU):
            i = WU * g + k
            l = CL * c + i
            for j in range(4):
                src[l, j, 7:8, :] = WRr[s, 0, j, pl.ds(l, 1), :]
                src[l, j, 40:41, :] = WRr[s, 1, j, pl.ds(l, 1), :]
        for k in range(WU):
            i = WU * g + k
            l = CL * c + i
            lm = jnp.maximum(l - 1, 0) if k == 0 else l - 1
            mid = [src[l, j, 8:40, :] for j in range(4)]
            edge = pltpu.roll(WC[...], lax.bitwise_and(128 - 2 * i, 127), 1)
            lo = [edge] + [pltpu.roll(m, 1, 1) for m in mid]
            hi = [pltpu.roll(m, 127, 1) for m in mid] + [edge]
            for j in range(4):
                y_lo = jnp.where(lane32 == 0, lo[j], lo[j + 1])
                y_hi = jnp.where(lane32 == 127, hi[j + 1], hi[j])
                near = (src[lm, j, 8:40, :] + src[l + 1, j, 8:40, :]) + (src[l, j, 7:39, :] + src[l, j, 9:41, :])
                near = near + (y_lo + y_hi)
                lanes = slice(128 * j, 128 * j + 128)
                new = mid[j] + D[l, :, lanes] * (near - 6.0 * mid[j])
                if k == 0:
                    new = new + jnp.where(l == 0, FX[j], 0.0)
                if s == STEPS - 1:
                    solid_out[l, :, lanes] = new
                else:
                    dst[l, j, 8:40, :] = new
                    WRs[s + 1, 0, j, pl.ds(l, 1), :] = new[0:1, :]
                    WRs[s + 1, 1, j, pl.ds(l, 1), :] = new[31:32, :]
        return acc

    def wall_chunk(s, c):
        for copy in wall_copies(s, c):
            copy.wait_recv()
        even = lax.bitwise_and(lane32, 1) == 0
        WC[...] = jnp.where(even, WCr[s, 0, c], pltpu.roll(WCr[s, 1, c], 126, 1))

        def body(g, acc):
            return wall_group(s, c, g, acc)

        acc = lax.fori_loop(0, CL // WU, body, zero32)
        if s < STEPS - 1:
            WCs[s + 1, c] = wall_pack(s, c, CL // WU - 1, acc)
            for copy in wall_copies(s + 1, c):
                copy.start()

    def wall_step(s, first, last, down):
        def body(n, carry):
            wall_chunk(s, CHUNKS - 1 - n if down else n)
            return carry

        lax.fori_loop(first, last, body, 0)

    def wall_flux():
        for piece, (dev, self_) in enumerate(sources):
            for part in PARTS:
                copy = face_copy(0, dev, piece, part, 0)
                here = self_
                if part == 0:
                    here = self_ & (gy > 0)
                if part == 2:
                    here = self_ & (gy < 3)
                pl.when(jnp.logical_not(here))(copy.wait_recv)
        tiles = [jnp.where(FB[1, j] > 0.5, FB[0, j], -FB[0, j]) for j in range(4)]
        prow = lax.broadcasted_iota(I32, (32, 128), 0)
        half = row * 16 + lax.shift_right_logical(prow, 1)
        for k in range(4):
            if k % 2 == 0:
                a, b, shift, cut = k // 2, k // 2 + 1, 32, 32
            else:
                a, b, shift, cut = k // 2 + 1, k // 2 + 2, 96, 96
            a, b = ((0, 1), (1, 2), (1, 2), (2, 3))[k]
            window = jnp.where(lane32 < cut, pltpu.roll(tiles[a], shift, 1), pltpu.roll(tiles[b], shift, 1))
            U[pl.ds(0, 32, stride=2), :] = window
            U[pl.ds(1, 32, stride=2), :] = window
            own = OW[:, 128 * k : 128 * k + 128]
            arow = lax.shift_right_logical(own, 10)
            acol = lax.bitwise_and(own, 1023)
            shift_row = lax.bitwise_and(arow - half + DISP, 511)
            col = lax.bitwise_and(acol - (gz * 256 - 128), 1023) - (96 + 64 * k)
            value = jnp.zeros((32, 128), F32)
            for d in range(2 * DISP + 1):
                base = 16 + 2 * (d - DISP)
                picked = jnp.take_along_axis(U[base : base + 32, :], col, axis=1, mode="promise_in_bounds")
                value = jnp.where(shift_row == d, picked, value)
            gas_at = jnp.abs(value)
            film = jnp.where(value > 0.0, 0.15 * jnp.exp(0.7 * jnp.log(gas_at)), 0.0)
            FX[k] = 0.25 * (film * (gas_at - S[0, 0, k, 8:40, :]))

    loads["v"].wait()
    for copy in g_copies:
        copy.wait_recv()
    GC[...] = jnp.where(lax.bitwise_and(lane64, 1) == 0, GCr[0], pltpu.roll(GCr[1], 126, 1))
    gas_layers(1, GAS_1)
    loads["d"].wait()
    loads["ow"].wait()
    wall_flux()
    wall_step(0, 0, CHUNKS, True)
    wall_step(1, 0, CHUNKS, True)
    gas_layers(GAS_1, GAS_2)
    wall_step(2, 0, CHUNKS, False)
    wall_chunk(3, 0)
    for j in range(4):
        T0[j] = solid_out[0, :, 128 * j : 128 * j + 128]

    lane16 = lane_iota(16)
    idx = lax.bitwise_and(2 * lane16, 127)
    for k in range(2):
        halves = []
        for j in (2 * k, 2 * k + 1):
            y = T0[j, pl.ds(0, 16, stride=2), :] + T0[j, pl.ds(1, 16, stride=2), :]
            y = 0.25 * (y + pltpu.roll(y, 127, 1))
            halves.append(jnp.take_along_axis(y, idx, axis=1, mode="promise_in_bounds"))
        WTs[k] = jnp.where(lane16 < 64, halves[0], halves[1])
    wt_self = (gz == 0) & (gy == 0)
    wt_rows = pl.ds(pl.multiple_of(gy * 16, 16), 16)
    wt_copy = send(WTs, WTr.at[:, wt_rows, :], t_send, t_recv.at[gy], (gx, gz, 0))
    pl.when(jnp.logical_not(wt_self))(wt_copy.start)

    @pl.when(wt_self)
    def _():
        WTr[:, 0:16, :] = WTs[...]

    wall_step(3, 1, CHUNKS, False)
    gas_layers(GAS_2, GL - 1)
    pl.when(jnp.logical_not(at_top))(z_down.wait_recv)

    @pl.when(at_top)
    def _():
        for f in range(2):
            for j in range(2):
                G[f, GL + 1, j, 8:72, :] = G[f, GL, j, 8:72, :]

    gas_layers(GL - 1, GL)

    @pl.when(jnp.logical_not(at_wall))
    def _():
        z_up.wait_recv()

    @pl.when(at_wall)
    def _():
        for t in range(4):
            copy = send(WTs, WTr.at[:, pl.ds(16 * t, 16), :], t_send, t_recv.at[t], (gx, t, gy))
            here = (gy == 0) & (t == 0)
            pl.when(jnp.logical_not(here))(copy.wait_recv)
        for j in range(2):
            temp = G[0, 1, j, 8:72, :]
            G[0, 0, j, 8:72, :] = jnp.where(FS[1, j] > 0.5, 2.0 * WTr[j] - temp, temp)
            G[1, 0, j, 8:72, :] = G[1, 1, j, 8:72, :]

    gas_layers(0, 1)

    for s in range(STEPS):
        for c in range(CHUNKS):
            for copy in wall_copies(s, c):
                copy.wait_send()
    for copy in g_copies:
        copy.wait_send()
    pl.when(jnp.logical_not(at_wall))(z_down.wait_send)
    pl.when(jnp.logical_not(at_top))(z_up.wait_send)
    pl.when(jnp.logical_not(wt_self))(wt_copy.wait_send)

    @pl.when(at_wall)
    def _():
        for n, (dev, piece, part, r, self_) in enumerate(face_targets()):
            copy = face_copy(n, dev, piece, part, r)
            if self_ is None:
                copy.wait_send()
            else:
                pl.when(jnp.logical_not(self_))(copy.wait_send)


def shards(gas_temp, fuel_frac, velocity, wall_flags, solid_temp, diffusivity, gas_owner):
    hbm = pl.BlockSpec(memory_space=pltpu.HBM)
    vmem = pl.BlockSpec(memory_space=pltpu.VMEM)
    gas_shape, solid_shape = gas_temp.shape, solid_temp.shape
    dma = pltpu.SemaphoreType.DMA
    buf = pltpu.VMEM
    results = [gas_shape, gas_shape, solid_shape]
    return pl.pallas_call(
        kernel,
        out_shape=[pltpu.VMEM(s, F32) for s in results],
        in_specs=[hbm] * 7,
        out_specs=[vmem] * 3,
        scratch_shapes=[
            buf((2, GL + 2, 2, 80, 128), F32),
            buf((3, GL, 64, 256), F32),
            buf((2, NL + 1, 4, 48, 128), F32),
            buf((NL, 32, 512), F32),
            buf((64, 256), I32),
            buf((32, 512), I32),
            buf((2, 2, 64, 128), F32),
            buf((2, 4, 32, 128), F32),
            buf((64, 128), F32),
            buf((4, 32, 128), F32),
            buf((STEPS, 2, 4, NL, 128), F32),
            buf((STEPS, 2, 4, NL, 128), F32),
            buf((STEPS, CHUNKS, 32, 128), F32),
            buf((STEPS, 2, CHUNKS, 32, 128), F32),
            buf((32, 128), F32),
            buf((2, 2, 2, GL, 128), F32),
            buf((2, 2, 2, GL, 128), F32),
            buf((64, 128), F32),
            buf((2, 64, 128), F32),
            buf((64, 128), F32),
            buf((4, 32, 128), F32),
            buf((2, 16, 128), F32),
            buf((2, 64, 128), F32),
            dma((12,)),
            dma((STEPS, CHUNKS, 4)),
            dma((STEPS, CHUNKS, 4)),
            dma((6,)),
            dma((6,)),
            dma((36,)),
            dma((3, 3)),
            dma,
            dma((4,)),
        ],
        compiler_params=pltpu.CompilerParams(
            collective_id=0, has_side_effects=True, vmem_limit_bytes=52 * 1024 * 1024
        ),
        name="section",
    )(gas_temp, fuel_frac, velocity, wall_flags, solid_temp, diffusivity, gas_owner)


def solution(mesh):
    placed = (
        P("gz", "gx", "gy"),
        P("gz", "gx", "gy"),
        P(None, "gz", "gx", "gy"),
        P("gx", "gy"),
        P(None, ("gx", "gy"), "gz"),
        P(None, ("gx", "gy"), "gz"),
        P(("gx", "gy"), "gz"),
    )
    return jax.shard_map(
        shards,
        mesh=mesh,
        in_specs=placed,
        out_specs=(P("gz", "gx", "gy"), P("gz", "gx", "gy"), P(None, ("gx", "gy"), "gz")),
        check_vma=False,
    )
```

```python
import functools

import jax
import jax.numpy as jnp
from jax import lax
from jax.experimental import pallas as pl
from jax.experimental.pallas import tpu as pltpu
from jax.sharding import PartitionSpec as P

MESH = pl.DeviceIdType.MESH
F32 = jnp.float32
I32 = jnp.int32

STEPS = 4
CHUNKS = 4
CL = 16
NL = 64
WU = 4
PU = 4
GAS = (12, 18, 24, 30)
GL = 32
DISP = 4

PIECES = ((0, 0), (1, 1), (2, -1))
PARTS = (0, 1, 2)


def lane_iota(rows):
    return lax.broadcasted_iota(I32, (rows, 128), 1)


def local(src, dst, sem):
    copy = pltpu.make_async_copy(src, dst, sem)
    copy.start()
    return copy


def kernel(
    gas_ref, fuel_ref, vel_ref, flags_ref, solid_ref, diff_ref, owner_ref,
    gas_out, fuel_out, solid_out,
    G, V, S, D, FL, OW, FS, FB, U, FX,
    WRs, WRr, WCs, WCr, WC, GRs, GRr, GCs, GCr, GC, T0, WTs, WTr,
    lsem, w_send, w_recv, g_send, g_recv, f_send, f_recv, t_send, t_recv,
):
    gx, gy, gz = lax.axis_index("gx"), lax.axis_index("gy"), lax.axis_index("gz")
    row = gx * 4 + gy

    def row_device(r):
        r = lax.rem(r + 32, 32)
        return (lax.div(r, 4), lax.rem(r, 4), gz)

    up_dev = row_device(row - 1)
    down_dev = row_device(row + 1)
    left_dev = (gx, gy, lax.rem(gz + 3, 4))
    right_dev = (gx, gy, lax.rem(gz + 1, 4))
    xm = lax.rem(gx + 7, 8)
    xp = lax.rem(gx + 1, 8)
    gxm_dev = (xm, gy, gz)
    gxp_dev = (xp, gy, gz)
    gym_dev = (gx, lax.rem(gy + 3, 4), gz)
    gyp_dev = (gx, lax.rem(gy + 1, 4), gz)

    loads = {}
    n = 0
    for j in range(4):
        loads["s", j] = local(
            solid_ref.at[:, :, pl.ds(128 * j, 128)], S.at[0, pl.ds(0, NL), j, pl.ds(8, 32), :], lsem.at[n]
        )
        n += 1
    for j in range(2):
        loads["g0", j] = local(
            gas_ref.at[:, :, pl.ds(128 * j, 128)], G.at[0, pl.ds(1, GL), j, pl.ds(8, 64), :], lsem.at[n]
        )
        n += 1
    loads["fl"] = local(flags_ref, FL, lsem.at[n])
    n += 1
    for j in range(2):
        loads["g1", j] = local(
            fuel_ref.at[:, :, pl.ds(128 * j, 128)], G.at[1, pl.ds(1, GL), j, pl.ds(8, 64), :], lsem.at[n]
        )
        n += 1
    loads["ow"] = local(owner_ref, OW, lsem.at[n])
    n += 1
    loads["v"] = local(vel_ref, V, lsem.at[n])
    n += 1
    loads["d"] = local(diff_ref, D, lsem.at[n])

    barrier = pltpu.get_barrier_semaphore()

    def greet(dev):
        pl.semaphore_signal(barrier, inc=1, device_id=dev, device_id_type=MESH)

    for dev in (up_dev, down_dev, left_dev, right_dev, gxm_dev, gxp_dev, gym_dev, gyp_dev):
        greet(dev)
    at_wall = gz == 0
    at_top = gz == 3

    def is_me(a, b, c):
        return (a == gx) & (b == gy) & (c == gz)

    def face_targets():
        out = []
        for piece, shift in PIECES:
            tz = lax.rem(gy + shift + 4, 4)
            for t in range(4):
                self_ = (t == gy) & (tz == 0)
                out.append(((gx, t, tz), piece, 1, 16 * t, self_))
                if t > 0:
                    out.append(((gx, t, tz), piece, 0, 16 * t - 8, self_))
                if t < 3:
                    out.append(((gx, t, tz), piece, 2, 16 * t + 16, self_))
            out.append(((xp, 0, tz), piece, 0, 56, None))
            out.append(((xm, 3, tz), piece, 2, 0, None))
        return out

    def face_devices():
        out = []
        for piece, shift in PIECES:
            tz = lax.rem(gy + shift + 4, 4)
            for t in range(4):
                out.append(((gx, t, tz), (t == gy) & (tz == 0)))
            out.append(((xp, 0, tz), None))
            out.append(((xm, 3, tz), None))
        return out

    count = I32(8)

    @pl.when(at_wall)
    def _():
        for dev, self_ in face_devices():
            if self_ is None:
                greet(dev)
            else:
                pl.when(jnp.logical_not(self_))(functools.partial(greet, dev))

    sources = []
    for piece, shift in PIECES:
        sy = lax.rem(gz - shift + 4, 4)
        self_ = (gz == 0) & (sy == gy)
        sources.append(((gx, sy, 0), self_))
        pl.when(jnp.logical_not(self_))(functools.partial(greet, (gx, sy, 0)))
        pl.when(gy == 0)(functools.partial(greet, (xm, sy, 0)))
        pl.when(gy == 3)(functools.partial(greet, (xp, sy, 0)))
        other = jnp.where(self_, 0, 1) + jnp.where((gy == 0) | (gy == 3), 1, 0)
        count = count + other
    self_sends = I32(0)
    for _, self_ in face_devices():
        if self_ is not None:
            self_sends = self_sends + jnp.where(self_, 1, 0)
    count = count + jnp.where(at_wall, 18 - self_sends, 0)

    S[0, NL] = jnp.ones((4, 48, 128), F32)
    S[1, NL] = jnp.ones((4, 48, 128), F32)

    def send(src, dst, ssem, rsem, dev):
        return pltpu.make_async_remote_copy(
            src_ref=src, dst_ref=dst, send_sem=ssem, recv_sem=rsem, device_id=dev, device_id_type=MESH
        )

    def wall_copies(s, c):
        rows = pl.ds(c * CL if isinstance(c, int) else pl.multiple_of(c * CL, CL), CL)
        return (
            send(WRs.at[s, 0, :, rows, :], WRr.at[s, 1, :, rows, :], w_send.at[0], w_recv.at[s, c, 1], up_dev),
            send(WRs.at[s, 1, :, rows, :], WRr.at[s, 0, :, rows, :], w_send.at[1], w_recv.at[s, c, 0], down_dev),
            send(WCs.at[s, c], WCr.at[s, 1, c], w_send.at[2], w_recv.at[s, c, 3], left_dev),
            send(WCs.at[s, c], WCr.at[s, 0, c], w_send.at[3], w_recv.at[s, c, 2], right_dev),
        )

    lane32 = lane_iota(32)
    lane64 = lane_iota(64)

    for j in range(4):
        loads["s", j].wait()

    zero32 = jnp.zeros((32, 128), F32)

    def columns(acc, first, last, i, lane):
        both = pltpu.roll(jnp.where(lane < 64, first, last), 2 * i + 1, 1)
        return jnp.where(lax.shift_right_arithmetic(lane, 1) == i, both, acc)

    def pack_chunk(c, carry):
        def pack(n, acc):
            for k in range(PU):
                i = PU * n + k
                l = CL * c + i
                for j in range(4):
                    WRs[0, 0, j, pl.ds(l, 1), :] = S[0, l, j, 8:9, :]
                    WRs[0, 1, j, pl.ds(l, 1), :] = S[0, l, j, 39:40, :]
                acc = columns(acc, S[0, l, 0, 8:40, :], S[0, l, 3, 8:40, :], i, lane32)
            return acc

        WCs[0, c] = lax.fori_loop(0, CL // PU, pack, zero32)
        return carry

    lax.fori_loop(0, CHUNKS, pack_chunk, 0)

    for key in (("g0", 0), ("g0", 1), "fl", ("g1", 0), ("g1", 1)):
        loads[key].wait()
    for j in range(2):
        FS[0, j] = G[0, 1, j, 8:72, :]
        FS[1, j] = FL[:, 128 * j : 128 * j + 128].astype(F32)

    def gpack(n, acc):
        for k in range(2):
            l = 2 * n + k
            for f in range(2):
                for j in range(2):
                    GRs[0, f, j, pl.ds(l, 1), :] = G[f, l + 1, j, 8:9, :]
                    GRs[1, f, j, pl.ds(l, 1), :] = G[f, l + 1, j, 71:72, :]
                acc = columns(acc, G[f, l + 1, 0, 8:72, :], G[f, l + 1, 1, 8:72, :], f * GL + l, lane64)
        return acc

    GCs[...] = lax.fori_loop(0, GL // 2, gpack, jnp.zeros((64, 128), F32))

    pl.semaphore_wait(barrier, count)

    def face_ref(buf, piece):
        return buf.at[:, pl.ds(1, 2)] if piece == 0 else buf.at[:, pl.ds(0 if piece == 1 else 3, 1)]

    def face_source(piece):
        return FS if piece == 0 else FS.at[:, pl.ds(1 if piece == 1 else 0, 1)]

    PART = ((0, 8), (8, 16), (24, 8))

    def face_copy(n, dev, piece, part, r):
        start, size = PART[part]
        return send(
            face_source(piece).at[:, :, pl.ds(r, size), :],
            face_ref(FB, piece).at[:, :, pl.ds(start, size), :],
            f_send.at[n],
            f_recv.at[piece, part],
            dev,
        )

    def face_here(piece, part, r):
        start, size = PART[part]
        if piece == 0:
            FB[:, 1:3, start : start + size, :] = FS[:, :, r : r + size, :]
        elif piece == 1:
            FB[:, 0, start : start + size, :] = FS[:, 1, r : r + size, :]
        else:
            FB[:, 3, start : start + size, :] = FS[:, 0, r : r + size, :]

    g_copies = (
        send(GRs.at[0], GRr.at[1], g_send.at[0], g_recv.at[1], gxm_dev),
        send(GRs.at[1], GRr.at[0], g_send.at[1], g_recv.at[0], gxp_dev),
        send(GCs, GCr.at[1], g_send.at[2], g_recv.at[3], gym_dev),
        send(GCs, GCr.at[0], g_send.at[3], g_recv.at[2], gyp_dev),
    )
    for copy in g_copies:
        copy.start()
    for c in range(CHUNKS):
        for copy in wall_copies(0, c):
            copy.start()

    @pl.when(at_wall)
    def _():
        for n, (dev, piece, part, r, self_) in enumerate(face_targets()):
            copy = face_copy(n, dev, piece, part, r)
            if self_ is None:
                copy.start()
            else:
                pl.when(jnp.logical_not(self_))(copy.start)
                pl.when(self_)(functools.partial(face_here, piece, part, r))

    z_down = send(
        G.at[:, 1, :, pl.ds(8, 64), :], G.at[:, GL + 1, :, pl.ds(8, 64), :], g_send.at[4], g_recv.at[5], left_dev
    )
    z_up = send(
        G.at[:, GL, :, pl.ds(8, 64), :], G.at[:, 0, :, pl.ds(8, 64), :], g_send.at[5], g_recv.at[4], right_dev
    )
    pl.when(jnp.logical_not(at_wall))(z_down.start)
    pl.when(jnp.logical_not(at_top))(z_up.start)

    def gas_layer(l):
        g = l + 1
        for f in range(2):
            for j in range(2):
                G[f, g, j, 7:8, :] = GRr[0, f, j, pl.ds(l, 1), :]
                G[f, g, j, 72:73, :] = GRr[1, f, j, pl.ds(l, 1), :]
        RB = 16
        lane = lane_iota(RB)
        for b in range(64 // RB):
            r0 = 8 + RB * b
            rows = slice(r0, r0 + RB)
            out = slice(RB * b, RB * b + RB)
            sums, advs, mids = {}, {}, {}
            vels = [[V[d, l, out, 128 * j : 128 * j + 128] for j in range(2)] for d in range(3)]
            for f in range(2):
                i = f * GL + l
                mid = [G[f, g, j, rows, :] for j in range(2)]
                edge = pltpu.roll(GC[out, :], lax.bitwise_and(128 - 2 * i, 127), 1)
                lo = [edge] + [pltpu.roll(m, 1, 1) for m in mid]
                hi = [pltpu.roll(m, 127, 1) for m in mid] + [edge]
                for j in range(2):
                    y_lo = jnp.where(lane == 0, lo[j], lo[j + 1])
                    y_hi = jnp.where(lane == 127, hi[j + 1], hi[j])
                    x_lo = G[f, g, j, r0 - 1 : r0 - 1 + RB, :]
                    x_hi = G[f, g, j, r0 + 1 : r0 + 1 + RB, :]
                    z_lo = G[f, g - 1, j, rows, :]
                    z_hi = G[f, g + 1, j, rows, :]
                    sums[f, j] = ((z_lo + z_hi) + (x_lo + x_hi)) + (y_lo + y_hi)
                    advs[f, j] = 0.5 * (
                        vels[0][j] * (z_hi - z_lo) + vels[1][j] * (x_hi - x_lo) + vels[2][j] * (y_hi - y_lo)
                    )
                    mids[f, j] = mid[j]
            for j in range(2):
                temp, fuel = mids[0, j], mids[1, j]
                reaction = fuel * jnp.exp(-4.0 / temp)
                lanes = slice(128 * j, 128 * j + 128)
                gas_out[l, out, lanes] = temp + 0.2 * (
                    0.2 * (sums[0, j] - 6.0 * temp) - advs[0, j] + 3.0 * reaction
                )
                fuel_out[l, out, lanes] = fuel + 0.2 * (
                    0.15 * (sums[1, j] - 6.0 * fuel) - advs[1, j] - reaction
                )

    def gas_layers(first, last):
        def body(l, carry):
            gas_layer(l)
            return carry

        lax.fori_loop(first, last, body, 0)

    def wall_pack(s, c, g, acc):
        dst = S.at[(s + 1) % 2]
        for k in range(WU):
            i = WU * g + k
            l = jnp.maximum(CL * c + i, 0)
            acc = columns(acc, dst[l, 0, 8:40, :], dst[l, 3, 8:40, :], i, lane32)
        return acc

    def wall_group(s, c, g, acc):
        src, dst = S.at[s % 2], S.at[(s + 1) % 2]
        if s < STEPS - 1:
            acc = wall_pack(s, c, g - 1, acc)
        for k in range(WU):
            i = WU * g + k
            l = CL * c + i
            for j in range(4):
                src[l, j, 7:8, :] = WRr[s, 0, j, pl.ds(l, 1), :]
                src[l, j, 40:41, :] = WRr[s, 1, j, pl.ds(l, 1), :]
        for k in range(WU):
            i = WU * g + k
            l = CL * c + i
            lm = jnp.maximum(l - 1, 0) if k == 0 else l - 1
            mid = [src[l, j, 8:40, :] for j in range(4)]
            edge = pltpu.roll(WC[...], lax.bitwise_and(128 - 2 * i, 127), 1)
            lo = [edge] + [pltpu.roll(m, 1, 1) for m in mid]
            hi = [pltpu.roll(m, 127, 1) for m in mid] + [edge]
            for j in range(4):
                y_lo = jnp.where(lane32 == 0, lo[j], lo[j + 1])
                y_hi = jnp.where(lane32 == 127, hi[j + 1], hi[j])
                near = (src[lm, j, 8:40, :] + src[l + 1, j, 8:40, :]) + (src[l, j, 7:39, :] + src[l, j, 9:41, :])
                near = near + (y_lo + y_hi)
                lanes = slice(128 * j, 128 * j + 128)
                new = mid[j] + D[l, :, lanes] * (near - 6.0 * mid[j])
                if k == 0:
                    new = new + jnp.where(l == 0, FX[j], 0.0)
                if s == STEPS - 1:
                    solid_out[l, :, lanes] = new
                else:
                    dst[l, j, 8:40, :] = new
                    WRs[s + 1, 0, j, pl.ds(l, 1), :] = new[0:1, :]
                    WRs[s + 1, 1, j, pl.ds(l, 1), :] = new[31:32, :]
        return acc

    def wall_chunk(s, c):
        for copy in wall_copies(s, c):
            copy.wait_recv()
        even = lax.bitwise_and(lane32, 1) == 0
        WC[...] = jnp.where(even, WCr[s, 0, c], pltpu.roll(WCr[s, 1, c], 126, 1))

        def body(g, acc):
            return wall_group(s, c, g, acc)

        acc = lax.fori_loop(0, CL // WU, body, zero32)
        if s < STEPS - 1:
            WCs[s + 1, c] = wall_pack(s, c, CL // WU - 1, acc)
            for copy in wall_copies(s + 1, c):
                copy.start()

    def wall_step(s, first, last, down):
        def body(n, carry):
            wall_chunk(s, CHUNKS - 1 - n if down else n)
            return carry

        lax.fori_loop(first, last, body, 0)

    def wall_flux():
        for piece, (dev, self_) in enumerate(sources):
            for part in PARTS:
                copy = face_copy(0, dev, piece, part, 0)
                here = self_
                if part == 0:
                    here = self_ & (gy > 0)
                if part == 2:
                    here = self_ & (gy < 3)
                pl.when(jnp.logical_not(here))(copy.wait_recv)
        tiles = [jnp.where(FB[1, j] > 0.5, FB[0, j], -FB[0, j]) for j in range(4)]
        prow = lax.broadcasted_iota(I32, (32, 128), 0)
        half = row * 16 + lax.shift_right_logical(prow, 1)
        for k in range(4):
            if k % 2 == 0:
                a, b, shift, cut = k // 2, k // 2 + 1, 32, 32
            else:
                a, b, shift, cut = k // 2 + 1, k // 2 + 2, 96, 96
            a, b = ((0, 1), (1, 2), (1, 2), (2, 3))[k]
            window = jnp.where(lane32 < cut, pltpu.roll(tiles[a], shift, 1), pltpu.roll(tiles[b], shift, 1))
            U[pl.ds(0, 32, stride=2), :] = window
            U[pl.ds(1, 32, stride=2), :] = window
            own = OW[:, 128 * k : 128 * k + 128]
            arow = lax.shift_right_logical(own, 10)
            acol = lax.bitwise_and(own, 1023)
            shift_row = lax.bitwise_and(arow - half + DISP, 511)
            col = lax.bitwise_and(acol - (gz * 256 - 128), 1023) - (96 + 64 * k)
            value = jnp.zeros((32, 128), F32)
            for d in range(2 * DISP + 1):
                base = 16 + 2 * (d - DISP)
                picked = jnp.take_along_axis(U[base : base + 32, :], col, axis=1, mode="promise_in_bounds")
                value = jnp.where(shift_row == d, picked, value)
            gas_at = jnp.abs(value)
            film = jnp.where(value > 0.0, 0.15 * jnp.exp(0.7 * jnp.log(gas_at)), 0.0)
            FX[k] = 0.25 * (film * (gas_at - S[0, 0, k, 8:40, :]))

    loads["v"].wait()
    for copy in g_copies:
        copy.wait_recv()
    GC[...] = jnp.where(lax.bitwise_and(lane64, 1) == 0, GCr[0], pltpu.roll(GCr[1], 126, 1))
    gas_layers(1, GAS[0])
    loads["d"].wait()
    loads["ow"].wait()
    wall_flux()
    wall_step(0, 0, CHUNKS, False)
    gas_layers(GAS[0], GAS[1])
    wall_step(1, 0, CHUNKS, False)
    gas_layers(GAS[1], GAS[2])
    wall_step(2, 0, CHUNKS, False)
    gas_layers(GAS[2], GAS[3])
    wall_chunk(3, 0)
    for j in range(4):
        T0[j] = solid_out[0, :, 128 * j : 128 * j + 128]

    lane16 = lane_iota(16)
    idx = lax.bitwise_and(2 * lane16, 127)
    for k in range(2):
        halves = []
        for j in (2 * k, 2 * k + 1):
            y = T0[j, pl.ds(0, 16, stride=2), :] + T0[j, pl.ds(1, 16, stride=2), :]
            y = 0.25 * (y + pltpu.roll(y, 127, 1))
            halves.append(jnp.take_along_axis(y, idx, axis=1, mode="promise_in_bounds"))
        WTs[k] = jnp.where(lane16 < 64, halves[0], halves[1])
    wt_self = (gz == 0) & (gy == 0)
    wt_rows = pl.ds(pl.multiple_of(gy * 16, 16), 16)
    wt_copy = send(WTs, WTr.at[:, wt_rows, :], t_send, t_recv.at[gy], (gx, gz, 0))
    pl.when(jnp.logical_not(wt_self))(wt_copy.start)

    @pl.when(wt_self)
    def _():
        WTr[:, 0:16, :] = WTs[...]

    wall_step(3, 1, CHUNKS, False)
    gas_layers(GAS[3], GL - 1)
    pl.when(jnp.logical_not(at_top))(z_down.wait_recv)

    @pl.when(at_top)
    def _():
        for f in range(2):
            for j in range(2):
                G[f, GL + 1, j, 8:72, :] = G[f, GL, j, 8:72, :]

    gas_layers(GL - 1, GL)

    @pl.when(jnp.logical_not(at_wall))
    def _():
        z_up.wait_recv()

    @pl.when(at_wall)
    def _():
        for t in range(4):
            copy = send(WTs, WTr.at[:, pl.ds(16 * t, 16), :], t_send, t_recv.at[t], (gx, t, gy))
            here = (gy == 0) & (t == 0)
            pl.when(jnp.logical_not(here))(copy.wait_recv)
        for j in range(2):
            temp = G[0, 1, j, 8:72, :]
            G[0, 0, j, 8:72, :] = jnp.where(FS[1, j] > 0.5, 2.0 * WTr[j] - temp, temp)
            G[1, 0, j, 8:72, :] = G[1, 1, j, 8:72, :]

    gas_layers(0, 1)

    send(WRs.at[:, 0], WRr.at[:, 1], w_send.at[0], w_recv.at[0, 0, 1], up_dev).wait_send()
    send(WRs.at[:, 1], WRr.at[:, 0], w_send.at[1], w_recv.at[0, 0, 0], down_dev).wait_send()
    send(WCs, WCr.at[:, 1], w_send.at[2], w_recv.at[0, 0, 3], left_dev).wait_send()
    send(WCs, WCr.at[:, 0], w_send.at[3], w_recv.at[0, 0, 2], right_dev).wait_send()
    for copy in g_copies:
        copy.wait_send()
    pl.when(jnp.logical_not(at_wall))(z_down.wait_send)
    pl.when(jnp.logical_not(at_top))(z_up.wait_send)
    pl.when(jnp.logical_not(wt_self))(wt_copy.wait_send)

    @pl.when(at_wall)
    def _():
        for n, (dev, piece, part, r, self_) in enumerate(face_targets()):
            copy = face_copy(n, dev, piece, part, r)
            if self_ is None:
                copy.wait_send()
            else:
                pl.when(jnp.logical_not(self_))(copy.wait_send)


def writer(a_ref, b_ref, c_ref, a_out, b_out, c_out, sems):
    copies = []
    for src, dst in ((a_ref, a_out), (b_ref, b_out), (c_ref, c_out)):
        part = src.shape[0] // 4
        for k in range(4):
            copies.append(local(src.at[pl.ds(k * part, part)], dst.at[pl.ds(k * part, part)], sems.at[len(copies)]))
    for copy in copies:
        copy.wait()


def shards(gas_temp, fuel_frac, velocity, wall_flags, solid_temp, diffusivity, gas_owner):
    hbm = pl.BlockSpec(memory_space=pltpu.HBM)
    vmem = pl.BlockSpec(memory_space=pltpu.VMEM)
    gas_shape, solid_shape = gas_temp.shape, solid_temp.shape
    dma = pltpu.SemaphoreType.DMA
    buf = pltpu.VMEM
    results = [gas_shape, gas_shape, solid_shape]
    results_here = pl.pallas_call(
        kernel,
        out_shape=[pltpu.VMEM(s, F32) for s in results],
        in_specs=[hbm] * 7,
        out_specs=[vmem] * 3,
        scratch_shapes=[
            buf((2, GL + 2, 2, 80, 128), F32),
            buf((3, GL, 64, 256), F32),
            buf((2, NL + 1, 4, 48, 128), F32),
            buf((NL, 32, 512), F32),
            buf((64, 256), I32),
            buf((32, 512), I32),
            buf((2, 2, 64, 128), F32),
            buf((2, 4, 32, 128), F32),
            buf((64, 128), F32),
            buf((4, 32, 128), F32),
            buf((STEPS, 2, 4, NL, 128), F32),
            buf((STEPS, 2, 4, NL, 128), F32),
            buf((STEPS, CHUNKS, 32, 128), F32),
            buf((STEPS, 2, CHUNKS, 32, 128), F32),
            buf((32, 128), F32),
            buf((2, 2, 2, GL, 128), F32),
            buf((2, 2, 2, GL, 128), F32),
            buf((64, 128), F32),
            buf((2, 64, 128), F32),
            buf((64, 128), F32),
            buf((4, 32, 128), F32),
            buf((2, 16, 128), F32),
            buf((2, 64, 128), F32),
            dma((12,)),
            dma((4,)),
            dma((STEPS, CHUNKS, 4)),
            dma((6,)),
            dma((6,)),
            dma((36,)),
            dma((3, 3)),
            dma,
            dma((4,)),
        ],
        compiler_params=pltpu.CompilerParams(
            collective_id=0, has_side_effects=True, vmem_limit_bytes=52 * 1024 * 1024
        ),
        name="section",
    )(gas_temp, fuel_frac, velocity, wall_flags, solid_temp, diffusivity, gas_owner)
    results_here = [pltpu.with_memory_space_constraint(r, pltpu.VMEM) for r in results_here]
    return pl.pallas_call(
        writer,
        out_shape=[jax.ShapeDtypeStruct(s, F32) for s in results],
        in_specs=[vmem] * 3,
        out_specs=[hbm] * 3,
        scratch_shapes=[dma((12,))],
        compiler_params=pltpu.CompilerParams(vmem_limit_bytes=2 * 1024 * 1024),
        name="writer",
    )(*results_here)


def solution(mesh):
    placed = (
        P("gz", "gx", "gy"),
        P("gz", "gx", "gy"),
        P(None, "gz", "gx", "gy"),
        P("gx", "gy"),
        P(None, ("gx", "gy"), "gz"),
        P(None, ("gx", "gy"), "gz"),
        P(("gx", "gy"), "gz"),
    )
    return jax.shard_map(
        shards,
        mesh=mesh,
        in_specs=placed,
        out_specs=(P("gz", "gx", "gy"), P("gz", "gx", "gy"), P(None, ("gx", "gy"), "gz")),
        check_vma=False,
    )
```

```python
import functools

import jax
import jax.numpy as jnp
from jax import lax
from jax.experimental import pallas as pl
from jax.experimental.pallas import tpu as pltpu
from jax.sharding import PartitionSpec as P

MESH = pl.DeviceIdType.MESH
F32 = jnp.float32
I32 = jnp.int32

STEPS = 4
CHUNKS = 4
CL = 16
NL = 64
HU = 2
WU = 2 * HU
PU = 4
GAS = (1, 11, 21, 31)
EDGES = (1, 9, 31)
GL = 32
DISP = 4

PIECES = ((0, 0), (1, 1), (2, -1))
PARTS = (0, 1, 2)


def lane_iota(rows):
    return lax.broadcasted_iota(I32, (rows, 128), 1)


def local(src, dst, sem):
    copy = pltpu.make_async_copy(src, dst, sem)
    copy.start()
    return copy


def kernel(
    gas_ref, fuel_ref, vel_ref, flags_ref, solid_ref, diff_ref, owner_ref,
    gas_out, fuel_out, solid_out,
    G, V, S0, S1, D, FL, OW, FS, FB, U, FX,
    WRs, WRr, WCs, WCr, WC, RA, RB, GRs, GRr, GCs, GCr, GC, T0, WTs, WTr,
    lsem, w_send, w_recv, g_send, g_recv, f_send, f_recv, t_send, t_recv,
):
    gx, gy, gz = lax.axis_index("gx"), lax.axis_index("gy"), lax.axis_index("gz")
    row = gx * 4 + gy

    def row_device(r):
        r = lax.rem(r + 32, 32)
        return (lax.div(r, 4), lax.rem(r, 4), gz)

    up_dev = row_device(row - 1)
    down_dev = row_device(row + 1)
    left_dev = (gx, gy, lax.rem(gz + 3, 4))
    right_dev = (gx, gy, lax.rem(gz + 1, 4))
    xm = lax.rem(gx + 7, 8)
    xp = lax.rem(gx + 1, 8)
    gxm_dev = (xm, gy, gz)
    gxp_dev = (xp, gy, gz)
    gym_dev = (gx, lax.rem(gy + 3, 4), gz)
    gyp_dev = (gx, lax.rem(gy + 1, 4), gz)

    loads = {}
    for j in range(4):
        loads["s", j] = local(
            solid_ref.at[:, :, pl.ds(128 * j, 128)], S0.at[pl.ds(0, NL), j, pl.ds(8, 32), :], lsem.at[j]
        )
    for j in range(2):
        loads["f", j] = local(gas_ref.at[0, :, pl.ds(128 * j, 128)], FS.at[0, j], lsem.at[4 + j])
    loads["fl"] = local(flags_ref, FL, lsem.at[6])

    def later_loads():
        loads["d"] = local(diff_ref, D, lsem.at[7])
        loads["ow"] = local(owner_ref, OW, lsem.at[8])
        for f, ref in enumerate((gas_ref, fuel_ref)):
            for j in range(2):
                loads["g", f, j] = local(
                    ref.at[:, :, pl.ds(128 * j, 128)],
                    G.at[f, pl.ds(1, GL), j, pl.ds(8, 64), :],
                    lsem.at[9 + 2 * f + j],
                )
        loads["v"] = local(vel_ref, V, lsem.at[13])

    barrier = pltpu.get_barrier_semaphore()

    def greet(dev):
        pl.semaphore_signal(barrier, inc=1, device_id=dev, device_id_type=MESH)

    for dev in (up_dev, down_dev, left_dev, right_dev, gxm_dev, gxp_dev, gym_dev, gyp_dev):
        greet(dev)
    at_wall = gz == 0
    at_top = gz == 3

    def is_me(a, b, c):
        return (a == gx) & (b == gy) & (c == gz)

    def face_targets():
        out = []
        for piece, shift in PIECES:
            tz = lax.rem(gy + shift + 4, 4)
            for t in range(4):
                self_ = (t == gy) & (tz == 0)
                out.append(((gx, t, tz), piece, 1, 16 * t, self_))
                if t > 0:
                    out.append(((gx, t, tz), piece, 0, 16 * t - 8, self_))
                if t < 3:
                    out.append(((gx, t, tz), piece, 2, 16 * t + 16, self_))
            out.append(((xp, 0, tz), piece, 0, 56, None))
            out.append(((xm, 3, tz), piece, 2, 0, None))
        return out

    def face_devices():
        out = []
        for piece, shift in PIECES:
            tz = lax.rem(gy + shift + 4, 4)
            for t in range(4):
                out.append(((gx, t, tz), (t == gy) & (tz == 0)))
            out.append(((xp, 0, tz), None))
            out.append(((xm, 3, tz), None))
        return out

    count = I32(8)

    @pl.when(at_wall)
    def _():
        for dev, self_ in face_devices():
            if self_ is None:
                greet(dev)
            else:
                pl.when(jnp.logical_not(self_))(functools.partial(greet, dev))

    sources = []
    for piece, shift in PIECES:
        sy = lax.rem(gz - shift + 4, 4)
        self_ = (gz == 0) & (sy == gy)
        sources.append(((gx, sy, 0), self_))
        pl.when(jnp.logical_not(self_))(functools.partial(greet, (gx, sy, 0)))
        pl.when(gy == 0)(functools.partial(greet, (xm, sy, 0)))
        pl.when(gy == 3)(functools.partial(greet, (xp, sy, 0)))
        other = jnp.where(self_, 0, 1) + jnp.where((gy == 0) | (gy == 3), 1, 0)
        count = count + other
    self_sends = I32(0)
    for _, self_ in face_devices():
        if self_ is not None:
            self_sends = self_sends + jnp.where(self_, 1, 0)
    count = count + jnp.where(at_wall, 18 - self_sends, 0)

    SS = (S0, S1)
    for ref in SS:
        for k in range(2):
            ref[NL + k] = jnp.ones((4, 48, 128), F32)

    def send(src, dst, ssem, rsem, dev):
        return pltpu.make_async_remote_copy(
            src_ref=src, dst_ref=dst, send_sem=ssem, recv_sem=rsem, device_id=dev, device_id_type=MESH
        )

    def wall_copies(s, c):
        rows = pl.ds(c * CL if isinstance(c, int) else pl.multiple_of(c * CL, CL), CL)
        return (
            send(WRs.at[s, 0, :, rows, :], WRr.at[s, 1, :, rows, :], w_send.at[0], w_recv.at[s, c, 1], up_dev),
            send(WRs.at[s, 1, :, rows, :], WRr.at[s, 0, :, rows, :], w_send.at[1], w_recv.at[s, c, 0], down_dev),
            send(WCs.at[s, c], WCr.at[s, 1, c], w_send.at[2], w_recv.at[s, c, 3], left_dev),
            send(WCs.at[s, c], WCr.at[s, 0, c], w_send.at[3], w_recv.at[s, c, 2], right_dev),
        )

    lane32 = lane_iota(32)
    lane64 = lane_iota(64)

    for j in range(4):
        loads["s", j].wait()
    later_loads()

    zero32 = jnp.zeros((32, 128), F32)
    zero_row = jnp.zeros((1, 128), F32)

    def columns(acc, first, last, i, lane):
        both = pltpu.roll(jnp.where(lane < 64, first, last), 2 * i + 1, 1)
        return jnp.where(lax.shift_right_arithmetic(lane, 1) == i, both, acc)

    def pack_chunk(c, carry):
        def pack(n, acc):
            for k in range(PU):
                i = PU * n + k
                l = CL * c + i
                for j in range(4):
                    S0[l, j, 7:8, :] = zero_row
                    S0[l, j, 40:41, :] = zero_row
                    WRs[0, 0, j, pl.ds(l, 1), :] = S0[l, j, 8:9, :]
                    WRs[0, 1, j, pl.ds(l, 1), :] = S0[l, j, 39:40, :]
                acc = columns(acc, S0[l, 0, 8:40, :], S0[l, 3, 8:40, :], i, lane32)
            return acc

        WCs[0, c] = lax.fori_loop(0, CL // PU, pack, zero32)
        return carry

    lax.fori_loop(0, CHUNKS, pack_chunk, 0)

    for key in (("f", 0), ("f", 1), "fl"):
        loads[key].wait()
    for j in range(2):
        FS[1, j] = FL[:, 128 * j : 128 * j + 128].astype(F32)

    def gpack(n, acc):
        for k in range(2):
            l = 2 * n + k
            for f in range(2):
                for j in range(2):
                    G[f, l + 1, j, 7:8, :] = zero_row
                    G[f, l + 1, j, 72:73, :] = zero_row
                    GRs[0, f, j, pl.ds(l, 1), :] = G[f, l + 1, j, 8:9, :]
                    GRs[1, f, j, pl.ds(l, 1), :] = G[f, l + 1, j, 71:72, :]
                acc = columns(acc, G[f, l + 1, 0, 8:72, :], G[f, l + 1, 1, 8:72, :], f * GL + l, lane64)
        return acc

    def gas_layer(l, inner):
        g = l + 1
        for f in range(0 if inner else 2):
            for j in range(2):
                G[f, g, j, 7:8, :] = GRr[0, f, j, pl.ds(l, 1), :]
                G[f, g, j, 72:73, :] = GRr[1, f, j, pl.ds(l, 1), :]
        RB = 16
        lane = lane_iota(RB)
        for b in range(64 // RB):
            r0 = 8 + RB * b
            rows = slice(r0, r0 + RB)
            out = slice(RB * b, RB * b + RB)
            sums, advs, mids = {}, {}, {}
            vels = [[V[d, l, out, 128 * j : 128 * j + 128] for j in range(2)] for d in range(3)]
            for f in range(2):
                i = f * GL + l
                mid = [G[f, g, j, rows, :] for j in range(2)]
                edge = 0.0
                if not inner:
                    edge = pltpu.roll(GC[out, :], lax.bitwise_and(128 - 2 * i, 127), 1)
                lo = [edge] + [pltpu.roll(m, 1, 1) for m in mid]
                hi = [pltpu.roll(m, 127, 1) for m in mid] + [edge]
                for j in range(2):
                    y_lo = jnp.where(lane == 0, lo[j], lo[j + 1])
                    y_hi = jnp.where(lane == 127, hi[j + 1], hi[j])
                    x_lo = G[f, g, j, r0 - 1 : r0 - 1 + RB, :]
                    x_hi = G[f, g, j, r0 + 1 : r0 + 1 + RB, :]
                    z_lo = G[f, g - 1, j, rows, :]
                    z_hi = G[f, g + 1, j, rows, :]
                    sums[f, j] = ((z_lo + z_hi) + (x_lo + x_hi)) + (y_lo + y_hi)
                    advs[f, j] = 0.5 * (
                        vels[0][j] * (z_hi - z_lo) + vels[1][j] * (x_hi - x_lo) + vels[2][j] * (y_hi - y_lo)
                    )
                    mids[f, j] = mid[j]
            for j in range(2):
                temp, fuel = mids[0, j], mids[1, j]
                reaction = fuel * jnp.exp(-4.0 / temp)
                lanes = slice(128 * j, 128 * j + 128)
                gas_out[l, out, lanes] = temp + 0.2 * (
                    0.2 * (sums[0, j] - 6.0 * temp) - advs[0, j] + 3.0 * reaction
                )
                fuel_out[l, out, lanes] = fuel + 0.2 * (
                    0.15 * (sums[1, j] - 6.0 * fuel) - advs[1, j] - reaction
                )

    def gas_layers(first, last):
        def body(l, carry):
            gas_layer(l, True)
            return carry

        lax.fori_loop(first, last, body, 0)

    def gas_edges(first, last):
        def body(n, carry):
            for k in range(2):
                l = first + 2 * n + k
                for f, out, rate in ((0, gas_out, 0.04), (1, fuel_out, 0.03)):
                    edge = pltpu.roll(GC[...], lax.bitwise_and(128 - 2 * (f * GL + l), 127), 1)
                    for j in range(2):
                        lanes = slice(128 * j, 128 * j + 128)
                        speed = V[1, l, 0:1, lanes]
                        out[l, 0:1, lanes] = out[l, 0:1, lanes] + (rate + 0.1 * speed) * GRr[0, f, j, pl.ds(l, 1), :]
                        speed = V[1, l, 63:64, lanes]
                        out[l, 63:64, lanes] = out[l, 63:64, lanes] + (rate - 0.1 * speed) * GRr[1, f, j, pl.ds(l, 1), :]
                    speed = V[2, l, :, 0:128]
                    out[l, :, 0:128] = out[l, :, 0:128] + jnp.where(lane64 == 0, (rate + 0.1 * speed) * edge, 0.0)
                    speed = V[2, l, :, 128:256]
                    out[l, :, 128:256] = out[l, :, 128:256] + jnp.where(lane64 == 127, (rate - 0.1 * speed) * edge, 0.0)
            return carry

        lax.fori_loop(0, (last - first) // 2, body, 0)

    pl.semaphore_wait(barrier, count)

    def face_ref(buf, piece):
        return buf.at[:, pl.ds(1, 2)] if piece == 0 else buf.at[:, pl.ds(0 if piece == 1 else 3, 1)]

    def face_source(piece):
        return FS if piece == 0 else FS.at[:, pl.ds(1 if piece == 1 else 0, 1)]

    PART = ((0, 8), (8, 16), (24, 8))

    def face_copy(n, dev, piece, part, r):
        start, size = PART[part]
        return send(
            face_source(piece).at[:, :, pl.ds(r, size), :],
            face_ref(FB, piece).at[:, :, pl.ds(start, size), :],
            f_send.at[n],
            f_recv.at[piece, part],
            dev,
        )

    def face_here(piece, part, r):
        start, size = PART[part]
        if piece == 0:
            FB[:, 1:3, start : start + size, :] = FS[:, :, r : r + size, :]
        elif piece == 1:
            FB[:, 0, start : start + size, :] = FS[:, 1, r : r + size, :]
        else:
            FB[:, 3, start : start + size, :] = FS[:, 0, r : r + size, :]

    g_copies = (
        send(GRs.at[0], GRr.at[1], g_send.at[0], g_recv.at[1], gxm_dev),
        send(GRs.at[1], GRr.at[0], g_send.at[1], g_recv.at[0], gxp_dev),
        send(GCs, GCr.at[1], g_send.at[2], g_recv.at[3], gym_dev),
        send(GCs, GCr.at[0], g_send.at[3], g_recv.at[2], gyp_dev),
    )
    for c in range(CHUNKS):
        for copy in wall_copies(0, c):
            copy.start()

    @pl.when(at_wall)
    def _():
        for n, (dev, piece, part, r, self_) in enumerate(face_targets()):
            copy = face_copy(n, dev, piece, part, r)
            if self_ is None:
                copy.start()
            else:
                pl.when(jnp.logical_not(self_))(copy.start)
                pl.when(self_)(functools.partial(face_here, piece, part, r))

    z_down = send(
        G.at[:, 1, :, pl.ds(8, 64), :], G.at[:, GL + 1, :, pl.ds(8, 64), :], g_send.at[4], g_recv.at[5], left_dev
    )
    z_up = send(
        G.at[:, GL, :, pl.ds(8, 64), :], G.at[:, 0, :, pl.ds(8, 64), :], g_send.at[5], g_recv.at[4], right_dev
    )

    def wall_pack(s, c, g, acc):
        dst = SS[(s + 1) % 2]
        for k in range(WU):
            i = WU * g + k
            l = jnp.maximum(CL * c + i, 0)
            acc = columns(acc, dst[l, 0, 8:40, :], dst[l, 3, 8:40, :], i, lane32)
        return acc

    def wall_sides(s, R, l0):
        src = SS[s % 2]
        for k in range(HU):
            l = l0 + k
            mid = [src[l, j, 8:40, :] for j in range(4)]
            lo = [None] + [pltpu.roll(m, 1, 1) for m in mid]
            hi = [pltpu.roll(m, 127, 1) for m in mid] + [None]
            for j in range(4):
                y_lo = lo[j + 1] if j > 0 else jnp.where(lane32 == 0, 0.0, lo[1])
                y_hi = hi[j] if j < 3 else jnp.where(lane32 == 127, 0.0, hi[3])
                if j > 0:
                    y_lo = jnp.where(lane32 == 0, lo[j], y_lo)
                if j < 3:
                    y_hi = jnp.where(lane32 == 127, hi[j + 1], y_hi)
                R[k, j] = y_lo + y_hi

    def wall_half(s, c, i0, R, first, inner=False):
        src, dst = SS[s % 2], SS[(s + 1) % 2]
        for k in range(HU):
            i = i0 + k
            l = CL * c + i
            lm = jnp.maximum(l - 1, 0) if first and k == 0 else l - 1
            if not inner:
                edge = pltpu.roll(WC[...], lax.bitwise_and(128 - 2 * i, 127), 1)
            for j in (1, 2, 0, 3):
                mid = src[l, j, 8:40, :]
                near = (src[lm, j, 8:40, :] + src[l + 1, j, 8:40, :]) + (src[l, j, 7:39, :] + src[l, j, 9:41, :])
                near = near + R[k, j]
                if j == 0 and not inner:
                    near = near + jnp.where(lane32 == 0, edge, 0.0)
                if j == 3 and not inner:
                    near = near + jnp.where(lane32 == 127, edge, 0.0)
                lanes = slice(128 * j, 128 * j + 128)
                new = mid + D[l, :, lanes] * (near - 6.0 * mid)
                if first and k == 0 and not inner:
                    new = new + jnp.where(l == 0, FX[j], 0.0)
                if s == STEPS - 1:
                    solid_out[l, :, lanes] = new
                else:
                    dst[l, j, 8:40, :] = new
                    if not inner:
                        WRs[s + 1, 0, j, pl.ds(l, 1), :] = new[0:1, :]
                        WRs[s + 1, 1, j, pl.ds(l, 1), :] = new[31:32, :]

    def wall_inner():
        def body(n, carry):
            wall_sides(0, RB, WU * n + HU)
            wall_half(0, 0, WU * n, RA, True, True)
            wall_sides(0, RA, WU * n + WU)
            wall_half(0, 0, WU * n + HU, RB, False, True)
            return carry

        wall_sides(0, RA, 0)
        lax.fori_loop(0, NL // WU, body, 0)

    def wall_edges(c, g, acc):
        acc = wall_pack(0, c, g - 1, acc)
        for k in range(WU):
            i = WU * g + k
            l = CL * c + i
            edge = pltpu.roll(WC[...], lax.bitwise_and(128 - 2 * i, 127), 1)
            for j in (1, 2, 0, 3):
                lanes = slice(128 * j, 128 * j + 128)
                top = D[l, 0:1, lanes] * WRr[0, 0, j, pl.ds(l, 1), :]
                low = D[l, 31:32, lanes] * WRr[0, 1, j, pl.ds(l, 1), :]
                S1[l, j, 8:9, :] = S1[l, j, 8:9, :] + top
                S1[l, j, 39:40, :] = S1[l, j, 39:40, :] + low
                if k == 0:
                    S1[l, j, 8:40, :] = S1[l, j, 8:40, :] + jnp.where(l == 0, FX[j], 0.0)
                if j == 0:
                    S1[l, j, 8:40, :] = S1[l, j, 8:40, :] + jnp.where(lane32 == 0, D[l, :, lanes] * edge, 0.0)
                if j == 3:
                    S1[l, j, 8:40, :] = S1[l, j, 8:40, :] + jnp.where(lane32 == 127, D[l, :, lanes] * edge, 0.0)
                WRs[1, 0, j, pl.ds(l, 1), :] = S1[l, j, 8:9, :]
                WRs[1, 1, j, pl.ds(l, 1), :] = S1[l, j, 39:40, :]
        return acc

    def wall_group(s, c, g, acc):
        src = SS[s % 2]
        i0 = WU * g
        if s < STEPS - 1:
            acc = wall_pack(s, c, g - 1, acc)
        for k in range(WU):
            l = CL * c + i0 + k
            for j in range(4):
                src[l, j, 7:8, :] = WRr[s, 0, j, pl.ds(l, 1), :]
                src[l, j, 40:41, :] = WRr[s, 1, j, pl.ds(l, 1), :]
        wall_sides(s, RB, CL * c + i0 + HU)
        wall_half(s, c, i0, RA, True)
        wall_sides(s, RA, CL * c + i0 + WU)
        wall_half(s, c, i0 + HU, RB, False)
        return acc

    def wall_chunk(s, c):
        for copy in wall_copies(s, c):
            copy.wait_recv()
        even = lax.bitwise_and(lane32, 1) == 0
        WC[...] = jnp.where(even, WCr[s, 0, c], pltpu.roll(WCr[s, 1, c], 126, 1))

        def body(g, acc):
            return wall_edges(c, g, acc) if s == 0 else wall_group(s, c, g, acc)

        acc = lax.fori_loop(0, CL // WU, body, zero32)
        if s < STEPS - 1:
            WCs[s + 1, c] = wall_pack(s, c, CL // WU - 1, acc)
            for copy in wall_copies(s + 1, c):
                copy.start()

    def wall_step(s, first, last, down):
        def body(n, carry):
            wall_chunk(s, CHUNKS - 1 - n if down else n)
            return carry

        lax.fori_loop(first, last, body, 0)

    def wall_flux():
        for piece, (dev, self_) in enumerate(sources):
            for part in PARTS:
                copy = face_copy(0, dev, piece, part, 0)
                here = self_
                if part == 0:
                    here = self_ & (gy > 0)
                if part == 2:
                    here = self_ & (gy < 3)
                pl.when(jnp.logical_not(here))(copy.wait_recv)
        tiles = [jnp.where(FB[1, j] > 0.5, FB[0, j], -FB[0, j]) for j in range(4)]
        prow = lax.broadcasted_iota(I32, (32, 128), 0)
        half = row * 16 + lax.shift_right_logical(prow, 1)
        for k in range(4):
            if k % 2 == 0:
                a, b, shift, cut = k // 2, k // 2 + 1, 32, 32
            else:
                a, b, shift, cut = k // 2 + 1, k // 2 + 2, 96, 96
            a, b = ((0, 1), (1, 2), (1, 2), (2, 3))[k]
            window = jnp.where(lane32 < cut, pltpu.roll(tiles[a], shift, 1), pltpu.roll(tiles[b], shift, 1))
            U[pl.ds(0, 32, stride=2), :] = window
            U[pl.ds(1, 32, stride=2), :] = window
            own = OW[:, 128 * k : 128 * k + 128]
            arow = lax.shift_right_logical(own, 10)
            acol = lax.bitwise_and(own, 1023)
            shift_row = lax.bitwise_and(arow - half + DISP, 511)
            col = lax.bitwise_and(acol - (gz * 256 - 128), 1023) - (96 + 64 * k)
            value = jnp.zeros((32, 128), F32)
            for d in range(2 * DISP + 1):
                base = 16 + 2 * (d - DISP)
                picked = jnp.take_along_axis(U[base : base + 32, :], col, axis=1, mode="promise_in_bounds")
                value = jnp.where(shift_row == d, picked, value)
            gas_at = jnp.abs(value)
            film = jnp.where(value > 0.0, 0.15 * jnp.exp(0.7 * jnp.log(gas_at)), 0.0)
            FX[k] = 0.25 * (film * (gas_at - S0[0, k, 8:40, :]))

    loads["d"].wait()
    loads["ow"].wait()
    wall_inner()
    for f in range(2):
        for j in range(2):
            loads["g", f, j].wait()
    GCs[...] = lax.fori_loop(0, GL // 2, gpack, jnp.zeros((64, 128), F32))
    for copy in g_copies:
        copy.start()
    pl.when(jnp.logical_not(at_wall))(z_down.start)
    pl.when(jnp.logical_not(at_top))(z_up.start)
    loads["v"].wait()
    gas_layers(GAS[0], GAS[1])
    wall_flux()
    wall_step(0, 0, CHUNKS, False)
    wall_sides(1, RA, 0)
    gas_layers(GAS[1], GAS[2])
    wall_step(1, 0, CHUNKS, False)
    wall_sides(2, RA, 0)
    gas_layers(GAS[2], GAS[3])
    wall_step(2, 0, CHUNKS, False)
    wall_sides(3, RA, 0)
    for copy in g_copies:
        copy.wait_recv()
    GC[...] = jnp.where(lax.bitwise_and(lane64, 1) == 0, GCr[0], pltpu.roll(GCr[1], 126, 1))
    gas_edges(EDGES[0], EDGES[1])
    wall_chunk(3, 0)
    for j in range(4):
        T0[j] = solid_out[0, :, 128 * j : 128 * j + 128]

    lane16 = lane_iota(16)
    idx = lax.bitwise_and(2 * lane16, 127)
    for k in range(2):
        halves = []
        for j in (2 * k, 2 * k + 1):
            y = T0[j, pl.ds(0, 16, stride=2), :] + T0[j, pl.ds(1, 16, stride=2), :]
            y = 0.25 * (y + pltpu.roll(y, 127, 1))
            halves.append(jnp.take_along_axis(y, idx, axis=1, mode="promise_in_bounds"))
        WTs[k] = jnp.where(lane16 < 64, halves[0], halves[1])
    wt_self = (gz == 0) & (gy == 0)
    wt_rows = pl.ds(pl.multiple_of(gy * 16, 16), 16)
    wt_copy = send(WTs, WTr.at[:, wt_rows, :], t_send, t_recv.at[gy], (gx, gz, 0))
    pl.when(jnp.logical_not(wt_self))(wt_copy.start)

    @pl.when(wt_self)
    def _():
        WTr[:, 0:16, :] = WTs[...]

    wall_step(3, 1, CHUNKS, False)
    gas_edges(EDGES[1], EDGES[2])
    pl.when(jnp.logical_not(at_top))(z_down.wait_recv)

    @pl.when(at_top)
    def _():
        for f in range(2):
            for j in range(2):
                G[f, GL + 1, j, 8:72, :] = G[f, GL, j, 8:72, :]

    gas_layer(GL - 1, False)

    @pl.when(jnp.logical_not(at_wall))
    def _():
        z_up.wait_recv()

    @pl.when(at_wall)
    def _():
        for t in range(4):
            copy = send(WTs, WTr.at[:, pl.ds(16 * t, 16), :], t_send, t_recv.at[t], (gx, t, gy))
            here = (gy == 0) & (t == 0)
            pl.when(jnp.logical_not(here))(copy.wait_recv)
        for j in range(2):
            temp = G[0, 1, j, 8:72, :]
            G[0, 0, j, 8:72, :] = jnp.where(FS[1, j] > 0.5, 2.0 * WTr[j] - temp, temp)
            G[1, 0, j, 8:72, :] = G[1, 1, j, 8:72, :]

    gas_layer(0, False)

    send(WRs.at[:, 0], WRr.at[:, 1], w_send.at[0], w_recv.at[0, 0, 1], up_dev).wait_send()
    send(WRs.at[:, 1], WRr.at[:, 0], w_send.at[1], w_recv.at[0, 0, 0], down_dev).wait_send()
    send(WCs, WCr.at[:, 1], w_send.at[2], w_recv.at[0, 0, 3], left_dev).wait_send()
    send(WCs, WCr.at[:, 0], w_send.at[3], w_recv.at[0, 0, 2], right_dev).wait_send()
    for copy in g_copies:
        copy.wait_send()
    pl.when(jnp.logical_not(at_wall))(z_down.wait_send)
    pl.when(jnp.logical_not(at_top))(z_up.wait_send)
    pl.when(jnp.logical_not(wt_self))(wt_copy.wait_send)

    @pl.when(at_wall)
    def _():
        for n, (dev, piece, part, r, self_) in enumerate(face_targets()):
            copy = face_copy(n, dev, piece, part, r)
            if self_ is None:
                copy.wait_send()
            else:
                pl.when(jnp.logical_not(self_))(copy.wait_send)


def writer(a_ref, b_ref, c_ref, a_out, b_out, c_out, sems):
    copies = []
    for src, dst in ((a_ref, a_out), (b_ref, b_out), (c_ref, c_out)):
        part = src.shape[0] // 4
        for k in range(4):
            copies.append(local(src.at[pl.ds(k * part, part)], dst.at[pl.ds(k * part, part)], sems.at[len(copies)]))
    for copy in copies:
        copy.wait()


def shards(gas_temp, fuel_frac, velocity, wall_flags, solid_temp, diffusivity, gas_owner):
    hbm = pl.BlockSpec(memory_space=pltpu.HBM)
    vmem = pl.BlockSpec(memory_space=pltpu.VMEM)
    gas_shape, solid_shape = gas_temp.shape, solid_temp.shape
    dma = pltpu.SemaphoreType.DMA
    buf = pltpu.VMEM
    results = [gas_shape, gas_shape, solid_shape]
    results_here = pl.pallas_call(
        kernel,
        out_shape=[pltpu.VMEM(s, F32) for s in results],
        in_specs=[hbm] * 7,
        out_specs=[vmem] * 3,
        scratch_shapes=[
            buf((2, GL + 2, 2, 80, 128), F32),
            buf((3, GL, 64, 256), F32),
            buf((NL + 2, 4, 48, 128), F32),
            buf((NL + 2, 4, 48, 128), F32),
            buf((NL, 32, 512), F32),
            buf((64, 256), I32),
            buf((32, 512), I32),
            buf((2, 2, 64, 128), F32),
            buf((2, 4, 32, 128), F32),
            buf((64, 128), F32),
            buf((4, 32, 128), F32),
            buf((STEPS, 2, 4, NL, 128), F32),
            buf((STEPS, 2, 4, NL, 128), F32),
            buf((STEPS, CHUNKS, 32, 128), F32),
            buf((STEPS, 2, CHUNKS, 32, 128), F32),
            buf((32, 128), F32),
            buf((HU, 4, 32, 128), F32),
            buf((HU, 4, 32, 128), F32),
            buf((2, 2, 2, GL, 128), F32),
            buf((2, 2, 2, GL, 128), F32),
            buf((64, 128), F32),
            buf((2, 64, 128), F32),
            buf((64, 128), F32),
            buf((4, 32, 128), F32),
            buf((2, 16, 128), F32),
            buf((2, 64, 128), F32),
            dma((14,)),
            dma((4,)),
            dma((STEPS, CHUNKS, 4)),
            dma((6,)),
            dma((6,)),
            dma((36,)),
            dma((3, 3)),
            dma,
            dma((4,)),
        ],
        compiler_params=pltpu.CompilerParams(
            collective_id=0, has_side_effects=True, vmem_limit_bytes=52 * 1024 * 1024
        ),
        name="section",
    )(gas_temp, fuel_frac, velocity, wall_flags, solid_temp, diffusivity, gas_owner)
    results_here = [pltpu.with_memory_space_constraint(r, pltpu.VMEM) for r in results_here]
    return pl.pallas_call(
        writer,
        out_shape=[jax.ShapeDtypeStruct(s, F32) for s in results],
        in_specs=[vmem] * 3,
        out_specs=[hbm] * 3,
        scratch_shapes=[dma((12,))],
        compiler_params=pltpu.CompilerParams(vmem_limit_bytes=2 * 1024 * 1024),
        name="writer",
    )(*results_here)


def solution(mesh):
    placed = (
        P("gz", "gx", "gy"),
        P("gz", "gx", "gy"),
        P(None, "gz", "gx", "gy"),
        P("gx", "gy"),
        P(None, ("gx", "gy"), "gz"),
        P(None, ("gx", "gy"), "gz"),
        P(("gx", "gy"), "gz"),
    )
    return jax.shard_map(
        shards,
        mesh=mesh,
        in_specs=placed,
        out_specs=(P("gz", "gx", "gy"), P("gz", "gx", "gy"), P(None, ("gx", "gy"), "gz")),
        check_vma=False,
    )
```

```python
import functools

import jax
import jax.numpy as jnp
from jax import lax
from jax.experimental import pallas as pl
from jax.experimental.pallas import tpu as pltpu
from jax.sharding import PartitionSpec as P

MESH = pl.DeviceIdType.MESH
F32 = jnp.float32
I32 = jnp.int32

STEPS = 4
CHUNKS = 4
CL = 16
NL = 64
HU = 2
WU = 2 * HU
PU = 4
GAS = (1, 31)
EDGES = (1, 9, 31)
GL = 32
DISP = 4

PIECES = ((0, 0), (1, 1), (2, -1))
PARTS = (0, 1, 2)


def lane_iota(rows):
    return lax.broadcasted_iota(I32, (rows, 128), 1)


def local(src, dst, sem):
    copy = pltpu.make_async_copy(src, dst, sem)
    copy.start()
    return copy


def kernel(
    gas_ref, fuel_ref, vel_ref, flags_ref, solid_ref, diff_ref, owner_ref,
    gas_out, fuel_out, solid_out,
    G, V, S0, S1, D, FL, OW, FS, FB, U, FX,
    WRs, WRr, WCs, WCr, WC, RA, RB, GRs, GRr, GCs, GCr, GC, T0, WTs, WTr,
    lsem, w_send, w_recv, g_send, g_recv, f_send, f_recv, t_send, t_recv,
):
    gx, gy, gz = lax.axis_index("gx"), lax.axis_index("gy"), lax.axis_index("gz")
    row = gx * 4 + gy

    def row_device(r):
        r = lax.rem(r + 32, 32)
        return (lax.div(r, 4), lax.rem(r, 4), gz)

    up_dev = row_device(row - 1)
    down_dev = row_device(row + 1)
    left_dev = (gx, gy, lax.rem(gz + 3, 4))
    right_dev = (gx, gy, lax.rem(gz + 1, 4))
    xm = lax.rem(gx + 7, 8)
    xp = lax.rem(gx + 1, 8)
    gxm_dev = (xm, gy, gz)
    gxp_dev = (xp, gy, gz)
    gym_dev = (gx, lax.rem(gy + 3, 4), gz)
    gyp_dev = (gx, lax.rem(gy + 1, 4), gz)

    loads = {}
    for j in range(4):
        loads["s", j] = local(
            solid_ref.at[:, :, pl.ds(128 * j, 128)], S0.at[pl.ds(0, NL), j, pl.ds(8, 32), :], lsem.at[j]
        )
    for j in range(2):
        loads["f", j] = local(gas_ref.at[0, :, pl.ds(128 * j, 128)], FS.at[0, j], lsem.at[4 + j])
    loads["fl"] = local(flags_ref, FL, lsem.at[6])

    def later_loads():
        loads["d"] = local(diff_ref, D, lsem.at[7])
        loads["ow"] = local(owner_ref, OW, lsem.at[8])
        for f, ref in enumerate((gas_ref, fuel_ref)):
            for j in range(2):
                loads["g", f, j] = local(
                    ref.at[:, :, pl.ds(128 * j, 128)],
                    G.at[f, pl.ds(1, GL), j, pl.ds(8, 64), :],
                    lsem.at[9 + 2 * f + j],
                )
        loads["v"] = local(vel_ref, V, lsem.at[13])

    barrier = pltpu.get_barrier_semaphore()

    def greet(dev):
        pl.semaphore_signal(barrier, inc=1, device_id=dev, device_id_type=MESH)

    for dev in (up_dev, down_dev, left_dev, right_dev, gxm_dev, gxp_dev, gym_dev, gyp_dev):
        greet(dev)
    at_wall = gz == 0
    at_top = gz == 3

    def is_me(a, b, c):
        return (a == gx) & (b == gy) & (c == gz)

    def face_targets():
        out = []
        for piece, shift in PIECES:
            tz = lax.rem(gy + shift + 4, 4)
            for t in range(4):
                self_ = (t == gy) & (tz == 0)
                out.append(((gx, t, tz), piece, 1, 16 * t, self_))
                if t > 0:
                    out.append(((gx, t, tz), piece, 0, 16 * t - 8, self_))
                if t < 3:
                    out.append(((gx, t, tz), piece, 2, 16 * t + 16, self_))
            out.append(((xp, 0, tz), piece, 0, 56, None))
            out.append(((xm, 3, tz), piece, 2, 0, None))
        return out

    def face_devices():
        out = []
        for piece, shift in PIECES:
            tz = lax.rem(gy + shift + 4, 4)
            for t in range(4):
                out.append(((gx, t, tz), (t == gy) & (tz == 0)))
            out.append(((xp, 0, tz), None))
            out.append(((xm, 3, tz), None))
        return out

    count = I32(8)

    @pl.when(at_wall)
    def _():
        for dev, self_ in face_devices():
            if self_ is None:
                greet(dev)
            else:
                pl.when(jnp.logical_not(self_))(functools.partial(greet, dev))

    sources = []
    for piece, shift in PIECES:
        sy = lax.rem(gz - shift + 4, 4)
        self_ = (gz == 0) & (sy == gy)
        sources.append(((gx, sy, 0), self_))
        pl.when(jnp.logical_not(self_))(functools.partial(greet, (gx, sy, 0)))
        pl.when(gy == 0)(functools.partial(greet, (xm, sy, 0)))
        pl.when(gy == 3)(functools.partial(greet, (xp, sy, 0)))
        other = jnp.where(self_, 0, 1) + jnp.where((gy == 0) | (gy == 3), 1, 0)
        count = count + other
    self_sends = I32(0)
    for _, self_ in face_devices():
        if self_ is not None:
            self_sends = self_sends + jnp.where(self_, 1, 0)
    count = count + jnp.where(at_wall, 18 - self_sends, 0)

    SS = (S0, S1)
    for ref in SS:
        for k in range(2):
            ref[NL + k] = jnp.ones((4, 48, 128), F32)

    def send(src, dst, ssem, rsem, dev):
        return pltpu.make_async_remote_copy(
            src_ref=src, dst_ref=dst, send_sem=ssem, recv_sem=rsem, device_id=dev, device_id_type=MESH
        )

    def wall_copies(s, c):
        rows = pl.ds(c * CL if isinstance(c, int) else pl.multiple_of(c * CL, CL), CL)
        return (
            send(WRs.at[s, 0, :, rows, :], WRr.at[s, 1, :, rows, :], w_send.at[0], w_recv.at[s, c, 1], up_dev),
            send(WRs.at[s, 1, :, rows, :], WRr.at[s, 0, :, rows, :], w_send.at[1], w_recv.at[s, c, 0], down_dev),
            send(WCs.at[s, c], WCr.at[s, 1, c], w_send.at[2], w_recv.at[s, c, 3], left_dev),
            send(WCs.at[s, c], WCr.at[s, 0, c], w_send.at[3], w_recv.at[s, c, 2], right_dev),
        )

    lane32 = lane_iota(32)
    lane64 = lane_iota(64)

    for j in range(4):
        loads["s", j].wait()
    later_loads()

    zero32 = jnp.zeros((32, 128), F32)
    zero_row = jnp.zeros((1, 128), F32)

    def columns(acc, first, last, i, lane):
        both = pltpu.roll(jnp.where(lane < 64, first, last), 2 * i + 1, 1)
        return jnp.where(lax.shift_right_arithmetic(lane, 1) == i, both, acc)

    def pack_chunk(c, carry):
        def pack(n, acc):
            for k in range(PU):
                i = PU * n + k
                l = CL * c + i
                for j in range(4):
                    S0[l, j, 7:8, :] = zero_row
                    S0[l, j, 40:41, :] = zero_row
                    WRs[0, 0, j, pl.ds(l, 1), :] = S0[l, j, 8:9, :]
                    WRs[0, 1, j, pl.ds(l, 1), :] = S0[l, j, 39:40, :]
                acc = columns(acc, S0[l, 0, 8:40, :], S0[l, 3, 8:40, :], i, lane32)
            return acc

        WCs[0, c] = lax.fori_loop(0, CL // PU, pack, zero32)
        return carry

    lax.fori_loop(0, CHUNKS, pack_chunk, 0)

    for key in (("f", 0), ("f", 1), "fl"):
        loads[key].wait()
    for j in range(2):
        FS[1, j] = FL[:, 128 * j : 128 * j + 128].astype(F32)

    def gpack(n, acc):
        for k in range(2):
            l = 2 * n + k
            for f in range(2):
                for j in range(2):
                    G[f, l + 1, j, 7:8, :] = zero_row
                    G[f, l + 1, j, 72:73, :] = zero_row
                    GRs[0, f, j, pl.ds(l, 1), :] = G[f, l + 1, j, 8:9, :]
                    GRs[1, f, j, pl.ds(l, 1), :] = G[f, l + 1, j, 71:72, :]
                acc = columns(acc, G[f, l + 1, 0, 8:72, :], G[f, l + 1, 1, 8:72, :], f * GL + l, lane64)
        return acc

    def gas_layer(l, inner):
        g = l + 1
        for f in range(0 if inner else 2):
            for j in range(2):
                G[f, g, j, 7:8, :] = GRr[0, f, j, pl.ds(l, 1), :]
                G[f, g, j, 72:73, :] = GRr[1, f, j, pl.ds(l, 1), :]
        RB = 16
        lane = lane_iota(RB)
        for b in range(64 // RB):
            r0 = 8 + RB * b
            rows = slice(r0, r0 + RB)
            out = slice(RB * b, RB * b + RB)
            sums, advs, mids = {}, {}, {}
            vels = [[V[d, l, out, 128 * j : 128 * j + 128] for j in range(2)] for d in range(3)]
            for f in range(2):
                i = f * GL + l
                mid = [G[f, g, j, rows, :] for j in range(2)]
                edge = 0.0
                if not inner:
                    edge = pltpu.roll(GC[out, :], lax.bitwise_and(128 - 2 * i, 127), 1)
                lo = [edge] + [pltpu.roll(m, 1, 1) for m in mid]
                hi = [pltpu.roll(m, 127, 1) for m in mid] + [edge]
                for j in range(2):
                    y_lo = jnp.where(lane == 0, lo[j], lo[j + 1])
                    y_hi = jnp.where(lane == 127, hi[j + 1], hi[j])
                    x_lo = G[f, g, j, r0 - 1 : r0 - 1 + RB, :]
                    x_hi = G[f, g, j, r0 + 1 : r0 + 1 + RB, :]
                    z_lo = G[f, g - 1, j, rows, :]
                    z_hi = G[f, g + 1, j, rows, :]
                    sums[f, j] = ((z_lo + z_hi) + (x_lo + x_hi)) + (y_lo + y_hi)
                    advs[f, j] = 0.5 * (
                        vels[0][j] * (z_hi - z_lo) + vels[1][j] * (x_hi - x_lo) + vels[2][j] * (y_hi - y_lo)
                    )
                    mids[f, j] = mid[j]
            for j in range(2):
                temp, fuel = mids[0, j], mids[1, j]
                reaction = fuel * jnp.exp(-4.0 / temp)
                lanes = slice(128 * j, 128 * j + 128)
                gas_out[l, out, lanes] = temp + 0.2 * (
                    0.2 * (sums[0, j] - 6.0 * temp) - advs[0, j] + 3.0 * reaction
                )
                fuel_out[l, out, lanes] = fuel + 0.2 * (
                    0.15 * (sums[1, j] - 6.0 * fuel) - advs[1, j] - reaction
                )

    def gas_layers(first, last):
        def body(l, carry):
            gas_layer(l, True)
            return carry

        lax.fori_loop(first, last, body, 0)

    def gas_edges(first, last):
        def body(n, carry):
            for k in range(2):
                l = first + 2 * n + k
                for f, out, rate in ((0, gas_out, 0.04), (1, fuel_out, 0.03)):
                    edge = pltpu.roll(GC[...], lax.bitwise_and(128 - 2 * (f * GL + l), 127), 1)
                    for j in range(2):
                        lanes = slice(128 * j, 128 * j + 128)
                        speed = V[1, l, 0:1, lanes]
                        out[l, 0:1, lanes] = out[l, 0:1, lanes] + (rate + 0.1 * speed) * GRr[0, f, j, pl.ds(l, 1), :]
                        speed = V[1, l, 63:64, lanes]
                        out[l, 63:64, lanes] = out[l, 63:64, lanes] + (rate - 0.1 * speed) * GRr[1, f, j, pl.ds(l, 1), :]
                    speed = V[2, l, :, 0:128]
                    out[l, :, 0:128] = out[l, :, 0:128] + jnp.where(lane64 == 0, (rate + 0.1 * speed) * edge, 0.0)
                    speed = V[2, l, :, 128:256]
                    out[l, :, 128:256] = out[l, :, 128:256] + jnp.where(lane64 == 127, (rate - 0.1 * speed) * edge, 0.0)
            return carry

        lax.fori_loop(0, (last - first) // 2, body, 0)

    pl.semaphore_wait(barrier, count)

    def face_ref(buf, piece):
        return buf.at[:, pl.ds(1, 2)] if piece == 0 else buf.at[:, pl.ds(0 if piece == 1 else 3, 1)]

    def face_source(piece):
        return FS if piece == 0 else FS.at[:, pl.ds(1 if piece == 1 else 0, 1)]

    PART = ((0, 8), (8, 16), (24, 8))

    def face_copy(n, dev, piece, part, r):
        start, size = PART[part]
        return send(
            face_source(piece).at[:, :, pl.ds(r, size), :],
            face_ref(FB, piece).at[:, :, pl.ds(start, size), :],
            f_send.at[n],
            f_recv.at[piece, part],
            dev,
        )

    def face_here(piece, part, r):
        start, size = PART[part]
        if piece == 0:
            FB[:, 1:3, start : start + size, :] = FS[:, :, r : r + size, :]
        elif piece == 1:
            FB[:, 0, start : start + size, :] = FS[:, 1, r : r + size, :]
        else:
            FB[:, 3, start : start + size, :] = FS[:, 0, r : r + size, :]

    g_copies = (
        send(GRs.at[0], GRr.at[1], g_send.at[0], g_recv.at[1], gxm_dev),
        send(GRs.at[1], GRr.at[0], g_send.at[1], g_recv.at[0], gxp_dev),
        send(GCs, GCr.at[1], g_send.at[2], g_recv.at[3], gym_dev),
        send(GCs, GCr.at[0], g_send.at[3], g_recv.at[2], gyp_dev),
    )
    @pl.when(at_wall)
    def _():
        for n, (dev, piece, part, r, self_) in enumerate(face_targets()):
            copy = face_copy(n, dev, piece, part, r)
            if self_ is None:
                copy.start()
            else:
                pl.when(jnp.logical_not(self_))(copy.start)
                pl.when(self_)(functools.partial(face_here, piece, part, r))

    for c in range(CHUNKS):
        for copy in wall_copies(0, c):
            copy.start()

    z_down = send(
        G.at[:, 1, :, pl.ds(8, 64), :], G.at[:, GL + 1, :, pl.ds(8, 64), :], g_send.at[4], g_recv.at[5], left_dev
    )
    z_up = send(
        G.at[:, GL, :, pl.ds(8, 64), :], G.at[:, 0, :, pl.ds(8, 64), :], g_send.at[5], g_recv.at[4], right_dev
    )

    def wall_pack(s, c, g, acc):
        dst = SS[(s + 1) % 2]
        for k in range(WU):
            i = WU * g + k
            l = jnp.maximum(CL * c + i, 0)
            acc = columns(acc, dst[l, 0, 8:40, :], dst[l, 3, 8:40, :], i, lane32)
        return acc

    def wall_sides(s, R, l0):
        src = SS[s % 2]
        for k in range(HU):
            l = l0 + k
            mid = [src[l, j, 8:40, :] for j in range(4)]
            lo = [None] + [pltpu.roll(m, 1, 1) for m in mid]
            hi = [pltpu.roll(m, 127, 1) for m in mid] + [None]
            for j in range(4):
                y_lo = lo[j + 1] if j > 0 else jnp.where(lane32 == 0, 0.0, lo[1])
                y_hi = hi[j] if j < 3 else jnp.where(lane32 == 127, 0.0, hi[3])
                if j > 0:
                    y_lo = jnp.where(lane32 == 0, lo[j], y_lo)
                if j < 3:
                    y_hi = jnp.where(lane32 == 127, hi[j + 1], y_hi)
                R[k, j] = y_lo + y_hi

    def wall_half(s, c, i0, R, first, inner=False):
        src, dst = SS[s % 2], SS[(s + 1) % 2]
        for k in range(HU):
            i = i0 + k
            l = CL * c + i
            lm = jnp.maximum(l - 1, 0) if first and k == 0 else l - 1
            if not inner:
                edge = pltpu.roll(WC[...], lax.bitwise_and(128 - 2 * i, 127), 1)
            for j in (1, 2, 0, 3):
                mid = src[l, j, 8:40, :]
                near = (src[lm, j, 8:40, :] + src[l + 1, j, 8:40, :]) + (src[l, j, 7:39, :] + src[l, j, 9:41, :])
                near = near + R[k, j]
                if j == 0 and not inner:
                    near = near + jnp.where(lane32 == 0, edge, 0.0)
                if j == 3 and not inner:
                    near = near + jnp.where(lane32 == 127, edge, 0.0)
                lanes = slice(128 * j, 128 * j + 128)
                new = mid + D[l, :, lanes] * (near - 6.0 * mid)
                if first and k == 0 and not inner:
                    new = new + jnp.where(l == 0, FX[j], 0.0)
                if s == STEPS - 1:
                    solid_out[l, :, lanes] = new
                else:
                    dst[l, j, 8:40, :] = new
                    if not inner:
                        WRs[s + 1, 0, j, pl.ds(l, 1), :] = new[0:1, :]
                        WRs[s + 1, 1, j, pl.ds(l, 1), :] = new[31:32, :]

    def wall_inner():
        def body(n, carry):
            wall_sides(0, RB, WU * n + HU)
            wall_half(0, 0, WU * n, RA, True, True)
            wall_sides(0, RA, WU * n + WU)
            wall_half(0, 0, WU * n + HU, RB, False, True)
            return carry

        wall_sides(0, RA, 0)
        lax.fori_loop(0, NL // WU, body, 0)

    def wall_edges(c, g, acc):
        acc = wall_pack(0, c, g - 1, acc)
        for k in range(WU):
            i = WU * g + k
            l = CL * c + i
            edge = pltpu.roll(WC[...], lax.bitwise_and(128 - 2 * i, 127), 1)
            for j in (1, 2, 0, 3):
                lanes = slice(128 * j, 128 * j + 128)
                top = D[l, 0:1, lanes] * WRr[0, 0, j, pl.ds(l, 1), :]
                low = D[l, 31:32, lanes] * WRr[0, 1, j, pl.ds(l, 1), :]
                S1[l, j, 8:9, :] = S1[l, j, 8:9, :] + top
                S1[l, j, 39:40, :] = S1[l, j, 39:40, :] + low
                if k == 0:
                    S1[l, j, 8:40, :] = S1[l, j, 8:40, :] + jnp.where(l == 0, FX[j], 0.0)
                if j == 0:
                    S1[l, j, 8:40, :] = S1[l, j, 8:40, :] + jnp.where(lane32 == 0, D[l, :, lanes] * edge, 0.0)
                if j == 3:
                    S1[l, j, 8:40, :] = S1[l, j, 8:40, :] + jnp.where(lane32 == 127, D[l, :, lanes] * edge, 0.0)
                WRs[1, 0, j, pl.ds(l, 1), :] = S1[l, j, 8:9, :]
                WRs[1, 1, j, pl.ds(l, 1), :] = S1[l, j, 39:40, :]
        return acc

    def wall_group(s, c, g, acc):
        src = SS[s % 2]
        i0 = WU * g
        if s < STEPS - 1:
            acc = wall_pack(s, c, g - 1, acc)
        for k in range(WU):
            l = CL * c + i0 + k
            for j in range(4):
                src[l, j, 7:8, :] = WRr[s, 0, j, pl.ds(l, 1), :]
                src[l, j, 40:41, :] = WRr[s, 1, j, pl.ds(l, 1), :]
        wall_sides(s, RB, CL * c + i0 + HU)
        wall_half(s, c, i0, RA, True)
        wall_sides(s, RA, CL * c + i0 + WU)
        wall_half(s, c, i0 + HU, RB, False)
        return acc

    def wall_chunk(s, c):
        for copy in wall_copies(s, c):
            copy.wait_recv()
        even = lax.bitwise_and(lane32, 1) == 0
        WC[...] = jnp.where(even, WCr[s, 0, c], pltpu.roll(WCr[s, 1, c], 126, 1))

        def body(g, acc):
            return wall_edges(c, g, acc) if s == 0 else wall_group(s, c, g, acc)

        acc = lax.fori_loop(0, CL // WU, body, zero32)
        if s < STEPS - 1:
            WCs[s + 1, c] = wall_pack(s, c, CL // WU - 1, acc)
            for copy in wall_copies(s + 1, c):
                copy.start()

    def wall_step(s, first, last, down):
        def body(n, carry):
            wall_chunk(s, CHUNKS - 1 - n if down else n)
            return carry

        lax.fori_loop(first, last, body, 0)

    def wall_flux():
        for piece, (dev, self_) in enumerate(sources):
            for part in PARTS:
                copy = face_copy(0, dev, piece, part, 0)
                here = self_
                if part == 0:
                    here = self_ & (gy > 0)
                if part == 2:
                    here = self_ & (gy < 3)
                pl.when(jnp.logical_not(here))(copy.wait_recv)
        tiles = [jnp.where(FB[1, j] > 0.5, FB[0, j], -FB[0, j]) for j in range(4)]
        prow = lax.broadcasted_iota(I32, (32, 128), 0)
        half = row * 16 + lax.shift_right_logical(prow, 1)
        for k in range(4):
            if k % 2 == 0:
                a, b, shift, cut = k // 2, k // 2 + 1, 32, 32
            else:
                a, b, shift, cut = k // 2 + 1, k // 2 + 2, 96, 96
            a, b = ((0, 1), (1, 2), (1, 2), (2, 3))[k]
            window = jnp.where(lane32 < cut, pltpu.roll(tiles[a], shift, 1), pltpu.roll(tiles[b], shift, 1))
            U[pl.ds(0, 32, stride=2), :] = window
            U[pl.ds(1, 32, stride=2), :] = window
            own = OW[:, 128 * k : 128 * k + 128]
            arow = lax.shift_right_logical(own, 10)
            acol = lax.bitwise_and(own, 1023)
            shift_row = lax.bitwise_and(arow - half + DISP, 511)
            col = lax.bitwise_and(acol - (gz * 256 - 128), 1023) - (96 + 64 * k)
            value = jnp.zeros((32, 128), F32)
            for d in range(2 * DISP + 1):
                base = 16 + 2 * (d - DISP)
                picked = jnp.take_along_axis(U[base : base + 32, :], col, axis=1, mode="promise_in_bounds")
                value = jnp.where(shift_row == d, picked, value)
            gas_at = jnp.abs(value)
            film = jnp.where(value > 0.0, 0.15 * jnp.exp(0.7 * jnp.log(gas_at)), 0.0)
            FX[k] = 0.25 * (film * (gas_at - S0[0, k, 8:40, :]))

    loads["d"].wait()
    loads["ow"].wait()
    wall_inner()
    for f in range(2):
        for j in range(2):
            loads["g", f, j].wait()
    GCs[...] = lax.fori_loop(0, GL // 2, gpack, jnp.zeros((64, 128), F32))
    for copy in g_copies:
        copy.start()
    pl.when(jnp.logical_not(at_wall))(z_down.start)
    pl.when(jnp.logical_not(at_top))(z_up.start)
    loads["v"].wait()
    gas_layers(GAS[0], GAS[1])
    wall_flux()
    wall_step(0, 0, CHUNKS, False)
    wall_sides(1, RA, 0)
    wall_step(1, 0, CHUNKS, False)
    wall_sides(2, RA, 0)
    wall_step(2, 0, CHUNKS, False)
    wall_sides(3, RA, 0)
    for copy in g_copies:
        copy.wait_recv()
    GC[...] = jnp.where(lax.bitwise_and(lane64, 1) == 0, GCr[0], pltpu.roll(GCr[1], 126, 1))
    gas_edges(EDGES[0], EDGES[1])
    wall_chunk(3, 0)
    for j in range(4):
        T0[j] = solid_out[0, :, 128 * j : 128 * j + 128]

    lane16 = lane_iota(16)
    idx = lax.bitwise_and(2 * lane16, 127)
    for k in range(2):
        halves = []
        for j in (2 * k, 2 * k + 1):
            y = T0[j, pl.ds(0, 16, stride=2), :] + T0[j, pl.ds(1, 16, stride=2), :]
            y = 0.25 * (y + pltpu.roll(y, 127, 1))
            halves.append(jnp.take_along_axis(y, idx, axis=1, mode="promise_in_bounds"))
        WTs[k] = jnp.where(lane16 < 64, halves[0], halves[1])
    wt_self = (gz == 0) & (gy == 0)
    wt_rows = pl.ds(pl.multiple_of(gy * 16, 16), 16)
    wt_copy = send(WTs, WTr.at[:, wt_rows, :], t_send, t_recv.at[gy], (gx, gz, 0))
    pl.when(jnp.logical_not(wt_self))(wt_copy.start)

    @pl.when(wt_self)
    def _():
        WTr[:, 0:16, :] = WTs[...]

    wall_step(3, 1, CHUNKS, False)
    gas_edges(EDGES[1], EDGES[2])
    pl.when(jnp.logical_not(at_top))(z_down.wait_recv)

    @pl.when(at_top)
    def _():
        for f in range(2):
            for j in range(2):
                G[f, GL + 1, j, 8:72, :] = G[f, GL, j, 8:72, :]

    gas_layer(GL - 1, False)

    @pl.when(jnp.logical_not(at_wall))
    def _():
        z_up.wait_recv()

    @pl.when(at_wall)
    def _():
        for t in range(4):
            copy = send(WTs, WTr.at[:, pl.ds(16 * t, 16), :], t_send, t_recv.at[t], (gx, t, gy))
            here = (gy == 0) & (t == 0)
            pl.when(jnp.logical_not(here))(copy.wait_recv)
        for j in range(2):
            temp = G[0, 1, j, 8:72, :]
            G[0, 0, j, 8:72, :] = jnp.where(FS[1, j] > 0.5, 2.0 * WTr[j] - temp, temp)
            G[1, 0, j, 8:72, :] = G[1, 1, j, 8:72, :]

    gas_layer(0, False)

    send(WRs.at[:, 0], WRr.at[:, 1], w_send.at[0], w_recv.at[0, 0, 1], up_dev).wait_send()
    send(WRs.at[:, 1], WRr.at[:, 0], w_send.at[1], w_recv.at[0, 0, 0], down_dev).wait_send()
    send(WCs, WCr.at[:, 1], w_send.at[2], w_recv.at[0, 0, 3], left_dev).wait_send()
    send(WCs, WCr.at[:, 0], w_send.at[3], w_recv.at[0, 0, 2], right_dev).wait_send()
    for copy in g_copies:
        copy.wait_send()
    pl.when(jnp.logical_not(at_wall))(z_down.wait_send)
    pl.when(jnp.logical_not(at_top))(z_up.wait_send)
    pl.when(jnp.logical_not(wt_self))(wt_copy.wait_send)

    @pl.when(at_wall)
    def _():
        for n, (dev, piece, part, r, self_) in enumerate(face_targets()):
            copy = face_copy(n, dev, piece, part, r)
            if self_ is None:
                copy.wait_send()
            else:
                pl.when(jnp.logical_not(self_))(copy.wait_send)


def writer(a_ref, b_ref, c_ref, a_out, b_out, c_out, sems):
    copies = []
    for src, dst in ((a_ref, a_out), (b_ref, b_out), (c_ref, c_out)):
        part = src.shape[0] // 4
        for k in range(4):
            copies.append(local(src.at[pl.ds(k * part, part)], dst.at[pl.ds(k * part, part)], sems.at[len(copies)]))
    for copy in copies:
        copy.wait()


def shards(gas_temp, fuel_frac, velocity, wall_flags, solid_temp, diffusivity, gas_owner):
    hbm = pl.BlockSpec(memory_space=pltpu.HBM)
    vmem = pl.BlockSpec(memory_space=pltpu.VMEM)
    gas_shape, solid_shape = gas_temp.shape, solid_temp.shape
    dma = pltpu.SemaphoreType.DMA
    buf = pltpu.VMEM
    results = [gas_shape, gas_shape, solid_shape]
    results_here = pl.pallas_call(
        kernel,
        out_shape=[pltpu.VMEM(s, F32) for s in results],
        in_specs=[hbm] * 7,
        out_specs=[vmem] * 3,
        scratch_shapes=[
            buf((2, GL + 2, 2, 80, 128), F32),
            buf((3, GL, 64, 256), F32),
            buf((NL + 2, 4, 48, 128), F32),
            buf((NL + 2, 4, 48, 128), F32),
            buf((NL, 32, 512), F32),
            buf((64, 256), I32),
            buf((32, 512), I32),
            buf((2, 2, 64, 128), F32),
            buf((2, 4, 32, 128), F32),
            buf((64, 128), F32),
            buf((4, 32, 128), F32),
            buf((STEPS, 2, 4, NL, 128), F32),
            buf((STEPS, 2, 4, NL, 128), F32),
            buf((STEPS, CHUNKS, 32, 128), F32),
            buf((STEPS, 2, CHUNKS, 32, 128), F32),
            buf((32, 128), F32),
            buf((HU, 4, 32, 128), F32),
            buf((HU, 4, 32, 128), F32),
            buf((2, 2, 2, GL, 128), F32),
            buf((2, 2, 2, GL, 128), F32),
            buf((64, 128), F32),
            buf((2, 64, 128), F32),
            buf((64, 128), F32),
            buf((4, 32, 128), F32),
            buf((2, 16, 128), F32),
            buf((2, 64, 128), F32),
            dma((14,)),
            dma((4,)),
            dma((STEPS, CHUNKS, 4)),
            dma((6,)),
            dma((6,)),
            dma((36,)),
            dma((3, 3)),
            dma,
            dma((4,)),
        ],
        compiler_params=pltpu.CompilerParams(
            collective_id=0, has_side_effects=True, vmem_limit_bytes=52 * 1024 * 1024
        ),
        name="section",
    )(gas_temp, fuel_frac, velocity, wall_flags, solid_temp, diffusivity, gas_owner)
    results_here = [pltpu.with_memory_space_constraint(r, pltpu.VMEM) for r in results_here]
    return pl.pallas_call(
        writer,
        out_shape=[jax.ShapeDtypeStruct(s, F32) for s in results],
        in_specs=[vmem] * 3,
        out_specs=[hbm] * 3,
        scratch_shapes=[dma((12,))],
        compiler_params=pltpu.CompilerParams(vmem_limit_bytes=2 * 1024 * 1024),
        name="writer",
    )(*results_here)


def solution(mesh):
    placed = (
        P("gz", "gx", "gy"),
        P("gz", "gx", "gy"),
        P(None, "gz", "gx", "gy"),
        P("gx", "gy"),
        P(None, ("gx", "gy"), "gz"),
        P(None, ("gx", "gy"), "gz"),
        P(("gx", "gy"), "gz"),
    )
    return jax.shard_map(
        shards,
        mesh=mesh,
        in_specs=placed,
        out_specs=(P("gz", "gx", "gy"), P("gz", "gx", "gy"), P(None, ("gx", "gy"), "gz")),
        check_vma=False,
    )
```
